32 devices in a mesh: dp: 4 (over y, z), tp: 8 (over x, core).
Axes of the slice: x: 4, y: 2, z: 2, core: 2. Of those that a mesh axis runs over, the one named last changes fastest.
The devices are a block of a 4x4x8 slice.
Arguments:
- hidden: bfloat16 [512, 2048], P('dp'), parts along dimension 0
- lengths: int32 [512], P('dp'), parts along dimension 0
- k_cache: bfloat16 [2, 512, 512, 8, 64], P(None, 'dp', None, 'tp'), parts along dimension 1
- v_cache: bfloat16 [2, 512, 512, 8, 64], P(None, 'dp', None, 'tp'), parts along dimension 1
- attn_norm: bfloat16 [2, 2048], replicated
- w_qkv: bfloat16 [2, 2048, 8, 384], P(None, None, 'tp')
- w_out: bfloat16 [2, 2048, 2048], P(None, 'tp')
- mlp_norm: bfloat16 [2, 2048], replicated
- w_gate: bfloat16 [2, 2048, 8192], P(None, None, 'tp')
- w_up: bfloat16 [2, 2048, 8192], P(None, None, 'tp')
- w_down: bfloat16 [2, 8192, 2048], P(None, 'tp')
Outputs:
- output: bfloat16 [512, 2048], P('dp'), parts along dimension 0
There are 4 independent parts. The reference program is written for one: setup_inputs(seed, part) draws one part's arguments, and reference() takes and returns one part's arrays. A program takes and returns all parts, laid end to end along the dimension named above; an argument that names none is the same for every part.
All inputs are finite; a program needn't handle non-finite values.
Results may differ from the reference program's by a relative error of at most 0.0186567.
Values are sent between devices in bfloat16 or wider.
A program may use at most 768 MiB of HBM per device.

```python
import jax
import jax.numpy as jnp
from jax import lax

D_MODEL = 2048
HEADS = 32
KV_HEADS = 8
HEAD_DIM = 64
FF_DIM = 8192
BATCH = 128
SEQ_LEN = 512
LAYERS = 2
GROUP_DEVS = 8
GROUP = HEADS // KV_HEADS
ROPE_BASE = 10000.0
NORM_EPS = 1e-5


def setup_inputs(seed: int = 0, part: int = 0) -> dict:
    base_key = jax.random.key(seed)
    part_key = jax.random.fold_in(base_key, part)
    keys = jax.random.split(part_key, 8)
    weight_keys = jax.random.split(base_key, 8)
    row_ids = jnp.arange(BATCH)
    long_count = max(1, BATCH // 8)
    long_len = jax.random.randint(keys[0], (BATCH,), SEQ_LEN // 2, SEQ_LEN)
    short_len = jax.random.randint(keys[1], (BATCH,), 1, SEQ_LEN // 16 + 1)
    lengths = jnp.where(row_ids < long_count, long_len, short_len)
    lengths = jnp.where(row_ids == 0, SEQ_LEN - 1, jnp.where(row_ids == BATCH - 1, 1, lengths)).astype(jnp.int32)
    hidden = jax.random.normal(keys[2], (BATCH, D_MODEL), jnp.float32).astype(jnp.bfloat16)
    cache_shape = (LAYERS, BATCH, SEQ_LEN, KV_HEADS, HEAD_DIM)
    mean_shape = (LAYERS, BATCH, 1, KV_HEADS, HEAD_DIM)
    k_cache = (1.5 * jax.random.normal(keys[3], cache_shape, jnp.float32)).astype(jnp.bfloat16)
    mean_live = jax.random.normal(keys[4], mean_shape, jnp.float32)
    mean_stale = jax.random.normal(keys[5], mean_shape, jnp.float32)
    live = jnp.arange(SEQ_LEN)[None, None, :, None, None] < lengths[None, :, None, None, None]
    noise = jax.random.normal(keys[6], cache_shape, jnp.float32)
    v_cache = (0.6 * jnp.where(live, mean_live, mean_stale) + 0.8 * noise).astype(jnp.bfloat16)
    qo_dim = HEADS * HEAD_DIM
    attn_norm = jax.random.uniform(weight_keys[0], (LAYERS, D_MODEL), jnp.float32, 0.5, 1.5).astype(jnp.bfloat16)
    w_qkv = (jax.random.normal(weight_keys[1], (LAYERS, D_MODEL, KV_HEADS, (GROUP + 2) * HEAD_DIM), jnp.float32) * D_MODEL ** -0.5).astype(jnp.bfloat16)
    w_out = (jax.random.normal(weight_keys[2], (LAYERS, qo_dim, D_MODEL), jnp.float32) * qo_dim ** -0.5).astype(jnp.bfloat16)
    mlp_norm = jax.random.uniform(weight_keys[3], (LAYERS, D_MODEL), jnp.float32, 0.5, 1.5).astype(jnp.bfloat16)
    w_gate = (jax.random.normal(weight_keys[4], (LAYERS, D_MODEL, FF_DIM), jnp.float32) * D_MODEL ** -0.5).astype(jnp.bfloat16)
    w_up = (jax.random.normal(weight_keys[5], (LAYERS, D_MODEL, FF_DIM), jnp.float32) * D_MODEL ** -0.5).astype(jnp.bfloat16)
    w_down = (jax.random.normal(weight_keys[6], (LAYERS, FF_DIM, D_MODEL), jnp.float32) * FF_DIM ** -0.5).astype(jnp.bfloat16)
    return {'hidden': hidden, 'lengths': lengths, 'k_cache': k_cache, 'v_cache': v_cache,
            'attn_norm': attn_norm, 'w_qkv': w_qkv, 'w_out': w_out, 'mlp_norm': mlp_norm,
            'w_gate': w_gate, 'w_up': w_up, 'w_down': w_down}


def rms_norm(values, gain):
    wide = values.astype(jnp.float32)
    scale = lax.rsqrt(jnp.mean(wide * wide, axis=-1, keepdims=True) + NORM_EPS)
    return (wide * scale * gain.astype(jnp.float32)).astype(jnp.bfloat16)


def rotate(values, cosine, sine):
    half = values.shape[-1] // 2
    first = values[..., :half]
    second = values[..., half:]
    return jnp.concatenate([first * cosine - second * sine, second * cosine + first * sine], axis=-1)


def attend_row(row_data):
    query, key_new, val_new, keys_row, values_row, length = row_data
    scale = HEAD_DIM ** -0.5
    query_wide = query.astype(jnp.float32)
    logits = jnp.einsum('kgd,skd->kgs', query_wide, keys_row.astype(jnp.float32)) * scale
    live = jnp.arange(SEQ_LEN) < length
    logits = jnp.where(live[None, None, :], logits, -1e30)
    self_logit = jnp.einsum('kgd,kd->kg', query_wide, key_new.astype(jnp.float32)) * scale
    peak = jnp.maximum(jnp.max(logits, axis=-1), self_logit)
    weights = jnp.exp(logits - peak[..., None]).astype(jnp.bfloat16).astype(jnp.float32)
    self_weight = jnp.exp(self_logit - peak).astype(jnp.bfloat16).astype(jnp.float32)
    denominator = jnp.sum(weights, axis=-1) + self_weight
    numerator = jnp.einsum('kgs,skd->kgd', weights, values_row.astype(jnp.float32))
    numerator = numerator + self_weight[..., None] * val_new.astype(jnp.float32)[:, None, :]
    return (numerator / denominator[..., None]).astype(jnp.bfloat16)


def reference(hidden, lengths, k_cache, v_cache, attn_norm, w_qkv, w_out, mlp_norm, w_gate, w_up, w_down):
    inv_freq = ROPE_BASE ** (-jnp.arange(0, HEAD_DIM, 2, dtype=jnp.float32) / HEAD_DIM)
    angles = lengths.astype(jnp.float32)[:, None] * inv_freq[None, :]
    cosine = jnp.cos(angles)
    sine = jnp.sin(angles)

    def layer_step(residual, layer_data):
        cache_k, cache_v, gain_attn, qkv_layer, out_layer, gain_mlp, gate_layer, up_layer, down_layer = layer_data
        normed = rms_norm(residual, gain_attn)
        fused = jnp.dot(normed, qkv_layer.reshape(D_MODEL, -1), preferred_element_type=jnp.float32).astype(jnp.bfloat16)
        fused = fused.reshape(BATCH, KV_HEADS, GROUP + 2, HEAD_DIM).astype(jnp.float32)
        query = rotate(fused[:, :, :GROUP], cosine[:, None, None, :], sine[:, None, None, :]).astype(jnp.bfloat16)
        key_new = rotate(fused[:, :, GROUP], cosine[:, None, :], sine[:, None, :]).astype(jnp.bfloat16)
        val_new = fused[:, :, GROUP + 1].astype(jnp.bfloat16)
        attended = lax.map(attend_row, (query, key_new, val_new, cache_k, cache_v, lengths))
        attended = attended.reshape(BATCH, GROUP_DEVS, -1).astype(jnp.float32)
        out_parts = jnp.einsum('btf,tfd->btd', attended, out_layer.reshape(GROUP_DEVS, -1, D_MODEL).astype(jnp.float32)).astype(jnp.bfloat16)
        after_attn = (residual.astype(jnp.float32) + jnp.sum(out_parts.astype(jnp.float32), axis=1)).astype(jnp.bfloat16)
        normed_mlp = rms_norm(after_attn, gain_mlp)
        gate_proj = jnp.dot(normed_mlp, gate_layer, preferred_element_type=jnp.float32).astype(jnp.bfloat16)
        up_proj = jnp.dot(normed_mlp, up_layer, preferred_element_type=jnp.float32).astype(jnp.bfloat16)
        activated = (jax.nn.silu(gate_proj.astype(jnp.float32)) * up_proj.astype(jnp.float32)).astype(jnp.bfloat16)
        activated = activated.reshape(BATCH, GROUP_DEVS, -1).astype(jnp.float32)
        down_parts = jnp.einsum('btf,tfd->btd', activated, down_layer.reshape(GROUP_DEVS, -1, D_MODEL).astype(jnp.float32)).astype(jnp.bfloat16)
        layer_out = (after_attn.astype(jnp.float32) + jnp.sum(down_parts.astype(jnp.float32), axis=1)).astype(jnp.bfloat16)
        return layer_out, None

    final, _ = lax.scan(layer_step, hidden, (k_cache, v_cache, attn_norm, w_qkv, w_out, mlp_norm, w_gate, w_up, w_down))
    return final
```

```python
import functools
import math

import jax
import jax.numpy as jnp
from jax import lax
from jax.experimental import pallas as pl
from jax.experimental.pallas import tpu as pltpu
from jax.sharding import PartitionSpec as P

ROPE_BASE = 10000.0
NORM_EPS = 1e-5
NEG = -1e30
TILE_ROWS = 16
F32 = jnp.float32
BF16 = jnp.bfloat16


def dot(a, b):
    return jnp.dot(a, b, preferred_element_type=F32)


class Comm:
    def __init__(self, send, recv):
        self.send, self.recv = send, recv
        self.sent, self.base, self.open = 0, 0, []

    def start(self, slot, src, dst, device):
        copy = pltpu.make_async_remote_copy(
            src_ref=src, dst_ref=dst, send_sem=self.send.at[self.sent], recv_sem=self.recv.at[self.base + slot],
            device_id={"tp": device}, device_id_type=pl.DeviceIdType.MESH)
        copy.start()
        self.sent += 1
        self.open.append(copy)

    def wait(self, slot, ref):
        pltpu.make_async_remote_copy(
            src_ref=ref, dst_ref=ref, send_sem=self.send.at[0], recv_sem=self.recv.at[self.base + slot],
            device_id={"tp": lax.axis_index("tp")}, device_id_type=pl.DeviceIdType.MESH).wait_recv()

    def drain(self):
        for copy in self.open:
            copy.wait_send()
        self.open = []


def kernel(group, layers,
           hidden, lengths, k_hbm, v_hbm, attn_norm, w_qkv, w_out, mlp_norm, w_gate, w_up, w_down, out,
           x_in, len_in, gains, wq, wo, wg, wu, wd, kbuf, vbuf,
           cos_tab, sin_tab, len_tab, qq, kz, vz, attn, normed, act,
           part, far_in, sib_in, own_in, near_in, rel_out, rel_in, xg,
           load_sem, k_sem, v_sem, send_sem, recv_sem):
    rows, d_model = hidden.shape
    half = rows // 2
    width = d_model // group
    chips = group // 2
    me = lax.axis_index("tp")
    chip, core = me // 2, me % 2
    sibling = chip * 2 + (1 - core)
    right, left, far = (chip + 1) % chips, (chip + chips - 1) % chips, (chip + 2) % chips
    n_tiles = rows // TILE_ROWS
    seq = kbuf.shape[2]
    head_dim = kbuf.shape[1]
    comm = Comm(send_sem, recv_sem)

    loads = []

    def load(src, dst):
        copy = pltpu.make_async_copy(src, dst, load_sem.at[len(loads)])
        copy.start()
        loads.append(copy)
        return copy

    def load_cache(layer):
        for i in range(n_tiles):
            rng = pl.ds(i * TILE_ROWS, TILE_ROWS)
            pltpu.make_async_copy(k_hbm.at[layer, rng], kbuf.at[rng], k_sem.at[i]).start()
            pltpu.make_async_copy(v_hbm.at[layer, rng], vbuf.at[rng], v_sem.at[i]).start()

    ld_len = load(lengths, len_in)
    ld_x = load(hidden, x_in)
    ld_gain = [load(attn_norm, gains.at[0]), load(mlp_norm, gains.at[1])]
    ld_q = [load(w_qkv.at[0], wq.at[0])]
    load_cache(0)
    ld_o = [load(w_out.at[0], wo.at[0])]
    ld_g, ld_u, ld_d = [], [], []

    barrier = pltpu.get_barrier_semaphore()
    for peer in (sibling, right * 2, right * 2 + 1, left * 2, left * 2 + 1):
        pl.semaphore_signal(barrier, inc=1, device_id={"tp": peer}, device_id_type=pl.DeviceIdType.MESH)
    pl.semaphore_wait(barrier, 5)

    ld_len.wait()
    len_row = jnp.broadcast_to(len_in[...].astype(F32), (rows, rows))
    len_tab[...] = len_row.T
    freq = lax.broadcasted_iota(jnp.int32, (head_dim // 2, rows), 0).astype(F32)
    angles = len_row[:head_dim // 2] * jnp.exp(freq * (-2.0 / head_dim * math.log(ROPE_BASE)))
    cosine, sine = jnp.cos(angles), jnp.sin(angles)
    cos_tab[...] = jnp.concatenate([cosine] * 4, axis=0).T
    sin_tab[...] = jnp.concatenate([-sine, sine, -sine, sine], axis=0).T

    def rms_norm(pieces, gain_row):
        total = jnp.zeros((rows, 1), F32)
        for i in range(group):
            wide = pieces(i)
            total = total + jnp.sum(wide * wide, axis=1, keepdims=True)
        scale = lax.rsqrt(total / d_model + NORM_EPS)
        for i in range(group):
            cols = slice(i * width, (i + 1) * width)
            normed[:, cols] = (pieces(i) * scale * gain_row(cols)).astype(BF16)

    def attention(layer):
        fused = dot(normed[...], wq[layer]).astype(BF16).astype(F32)
        lane = lax.broadcasted_iota(jnp.int32, (rows, 128), 1)
        first = lane % head_dim < head_dim // 2
        low = lane < head_dim
        cos, sin = cos_tab[...], sin_tab[...]

        def rope(x):
            swapped = jnp.where(first, pltpu.roll(x, 128 - head_dim // 2, 1), pltpu.roll(x, head_dim // 2, 1))
            return (x * cos + swapped * sin).astype(BF16).astype(F32)

        for pair in range(2):
            x = rope(fused[:, pair * 128:(pair + 1) * 128])
            swap = pltpu.roll(x, head_dim, 1)
            qq[2 * pair] = jnp.where(low, x, swap)
            qq[2 * pair + 1] = jnp.where(low, swap, x)
        kv = fused[:, 256:384]
        kz[...] = jnp.where(low, rope(kv), 0.0)
        vz[...] = pltpu.roll(kv, head_dim, 1)

        row16 = lax.broadcasted_iota(jnp.int32, (TILE_ROWS, 128), 0)
        high16 = lax.broadcasted_iota(jnp.int32, (TILE_ROWS, 128), 1) // head_dim
        pos = lax.broadcasted_iota(jnp.int32, (TILE_ROWS, seq), 1).astype(F32)
        col_row = lax.broadcasted_iota(jnp.int32, (head_dim, 4 * TILE_ROWS), 1) % TILE_ROWS

        def tile(i):
            rng = pl.ds(pl.multiple_of(i * TILE_ROWS, TILE_ROWS), TILE_ROWS)
            queries = [qq[g, rng, :] for g in range(4)]
            lhs = jnp.concatenate([
                jnp.concatenate([jnp.where(row16 == 2 * j + high16, q, 0.0).astype(BF16) for j in range(TILE_ROWS // 2)], axis=1)
                for q in queries], axis=0)
            pltpu.make_async_copy(k_hbm.at[layer, rng], kbuf.at[rng], k_sem.at[i]).wait()
            logits = dot(lhs, kbuf[rng].reshape(TILE_ROWS * head_dim, seq)) * head_dim ** -0.5
            live = pos < jnp.concatenate([len_tab[rng, :]] * (seq // 128), axis=1)
            keys = kz[rng, :]
            peaks, weights, sums, selfs = [], [], [], []
            for g in range(4):
                s = jnp.where(live, logits[g * TILE_ROWS:(g + 1) * TILE_ROWS], NEG)
                own = jnp.sum(queries[g] * keys, axis=1, keepdims=True) * head_dim ** -0.5
                peak = jnp.maximum(jnp.max(s, axis=1, keepdims=True), own)
                w = jnp.exp(s - peak).astype(BF16)
                w_own = jnp.exp(own - peak).astype(BF16).astype(F32)
                weights.append(w)
                selfs.append(w_own)
                sums.append(jnp.sum(w.astype(F32), axis=1, keepdims=True) + w_own)
            w_all = jnp.concatenate(weights, axis=0)
            pltpu.make_async_copy(v_hbm.at[layer, rng], vbuf.at[rng], v_sem.at[i]).wait()
            picked = lax.dot_general(vbuf[rng].reshape(TILE_ROWS * head_dim, seq), w_all, (((1,), (1,)), ((), ())),
                                     preferred_element_type=F32)
            numer = jnp.zeros((head_dim, 4 * TILE_ROWS), F32)
            for b in range(TILE_ROWS):
                numer = jnp.where(col_row == b, picked[b * head_dim:(b + 1) * head_dim], numer)
            numer = numer.T
            values = vz[rng, :][:, :head_dim]
            heads = [((numer[g * TILE_ROWS:(g + 1) * TILE_ROWS] + selfs[g] * values) / sums[g]).astype(BF16)
                     for g in range(4)]
            attn[rng, :] = jnp.concatenate(heads, axis=1)

        def body(i, carry):
            tile(2 * i)
            tile(2 * i + 1)
            return carry

        lax.fori_loop(0, n_tiles // 2, body, 0)

    def reduce_add(r, lhs, weight, own_rows):
        comm.base = r * SLOTS
        p, x = part.at[r], xg.at[r]
        top, bottom = pl.ds(0, half), pl.ds(half, half)

        def produce(index, target):
            cols = pl.ds(pl.multiple_of(target * 2 * width, 128), 2 * width)
            block = dot(lhs, weight[:, cols]).astype(BF16)
            p[index, 0] = block[:, :width]
            p[index, 1] = block[:, width:]

        produce(0, far)
        for k in range(2):
            comm.start(core, p.at[0, k, top], far_in.at[r, 0, core], right * 2 + k)
            comm.start(2 + core, p.at[0, k, bottom], far_in.at[r, 1, core], left * 2 + k)
        produce(1, right)
        comm.start(4, p.at[1, 1 - core, top], sib_in.at[r, 0], sibling)
        for k in range(2):
            comm.start(7 + core, p.at[1, k, bottom], near_in.at[r, 0, core], right * 2 + k)
        produce(2, left)
        comm.start(5, p.at[2, 1 - core, bottom], sib_in.at[r, 1], sibling)
        for k in range(2):
            comm.start(9 + core, p.at[2, k, top], near_in.at[r, 1, core], left * 2 + k)
        produce(3, chip)
        comm.start(6, p.at[3, 1 - core], own_in.at[r], sibling)

        for way, rng, target in ((0, top, right), (1, bottom, left)):
            for k in range(2):
                comm.wait(2 * way + k, far_in.at[r, way, k])
            comm.wait(4 + way, sib_in.at[r, way])
            rel_out[r, way] = (far_in[r, way, 0].astype(F32) + far_in[r, way, 1].astype(F32)
                               + p[1 + way, core, rng].astype(F32) + sib_in[r, way].astype(F32))
            comm.start(11 + way, rel_out.at[r, way], rel_in.at[r, way], target * 2 + core)

        comm.wait(6, own_in.at[r])
        mine = {}
        for rng in (top, bottom):
            mine[rng.start] = (own_rows(rng).astype(F32) + p[3, core, rng].astype(F32)
                               + own_in[r, rng].astype(F32))
        to_right, to_left = right * 2 + core, left * 2 + core
        for way, rng, slot, target in ((0, top, 13, to_right), (1, bottom, 14, to_left)):
            for k in range(2):
                comm.wait(7 + 2 * (1 - way) + k, near_in.at[r, 1 - way, k])
            comm.wait(11 + way, rel_in.at[r, way])
            total = (mine[rng.start] + near_in[r, 1 - way, 0].astype(F32) + near_in[r, 1 - way, 1].astype(F32)
                     + rel_in[r, way])
            x[me, rng] = total.astype(BF16)
            comm.start(slot, x.at[me, rng], x.at[me, rng], target)
        comm.start(15, x.at[me, top], x.at[me, top], to_left)
        comm.start(16, x.at[me, bottom], x.at[me, bottom], to_right)
        comm.start(19, x.at[me], x.at[me], sibling)
        from_left, from_right, from_far = left * 2 + core, right * 2 + core, far * 2 + core
        for slot, origin, rng, onward, target in (
                (13, from_left, top, 17, to_right), (14, from_right, bottom, 18, to_left),
                (15, from_right, top, None, None), (16, from_left, bottom, None, None),
                (17, from_far, top, None, None), (18, from_far, bottom, None, None)):
            piece = x.at[origin, rng]
            comm.wait(slot, piece)
            if onward is not None:
                comm.start(onward, piece, piece, target)
            comm.start(slot + 7, piece, piece, sibling)
        other = 1 - core
        comm.wait(19, x.at[sibling])
        for slot, origin, rng in ((20, left, top), (21, right, bottom), (22, right, top), (23, left, bottom),
                                  (24, far, top), (25, far, bottom)):
            comm.wait(slot, x.at[origin * 2 + other, rng])

    for layer in range(layers):
        if layer == 0:
            ld_x.wait()
            for copy in ld_gain:
                copy.wait()

        def gain(which):
            return lambda cols: gains[which, layer:layer + 1, cols].astype(F32)

        first = 2 * layer
        if layer == 0:
            rms_norm(lambda i: x_in[:, i * width:(i + 1) * width].astype(F32), gain(0))
            own_cols = pl.ds(pl.multiple_of(me * width, 128), width)
            own_rows = lambda rng: x_in[rng, own_cols]
        else:
            rms_norm(lambda i: xg[first - 1, i].astype(F32), gain(0))
            own_rows = lambda rng: xg[first - 1, me, rng]
        ld_q[layer].wait()
        attention(layer)
        if layer == 0:
            for at in range(layers):
                ld_g.append(load(w_gate.at[at], wg.at[at]))
                ld_u.append(load(w_up.at[at], wu.at[at]))
                ld_d.append(load(w_down.at[at], wd.at[at]))
                if at + 1 < layers:
                    ld_q.append(load(w_qkv.at[at + 1], wq.at[at + 1]))
                    load_cache(at + 1)
                    ld_o.append(load(w_out.at[at + 1], wo.at[at + 1]))
        ld_o[layer].wait()
        reduce_add(first, attn[...], wo.at[layer], own_rows)
        rms_norm(lambda i: xg[first, i].astype(F32), gain(1))
        ld_g[layer].wait()
        ld_u[layer].wait()
        n = normed[...]
        for c in range(0, act.shape[1], 256):
            g = dot(n, wg[layer, :, c:c + 256]).astype(BF16).astype(F32)
            u = dot(n, wu[layer, :, c:c + 256]).astype(BF16).astype(F32)
            act[:, c:c + 256] = (g * jax.nn.sigmoid(g) * u).astype(BF16)
        ld_d[layer].wait()
        reduce_add(first + 1, act[...], wd.at[layer], lambda rng: xg[first, me, rng])
    for i in range(group):
        out[:, i * width:(i + 1) * width] = xg[2 * layers - 1, i]
    comm.drain()


SLOTS = 26


def solution(mesh):
    group = mesh.shape["tp"]

    def local_step(hidden, lengths, k_cache, v_cache, attn_norm, w_qkv, w_out, mlp_norm, w_gate, w_up, w_down):
        rows, d_model = hidden.shape
        layers, _, seq, _, head_dim = k_cache.shape
        width = d_model // group
        half = rows // 2
        rounds = 2 * layers
        fused_width = w_qkv.shape[-1]
        n_tiles = rows // TILE_ROWS
        keys = jnp.transpose(k_cache, (0, 1, 3, 4, 2)).reshape(layers, rows, head_dim, seq)
        values = jnp.transpose(v_cache, (0, 1, 3, 4, 2)).reshape(layers, rows, head_dim, seq)
        w_qkv = w_qkv.reshape(layers, d_model, fused_width)
        any_spec = pl.BlockSpec(memory_space=pl.ANY)
        sem = pltpu.SemaphoreType.DMA
        n_loads = 4 + 5 * layers
        return pl.pallas_call(
            functools.partial(kernel, group, layers),
            out_shape=jax.ShapeDtypeStruct((rows, d_model), BF16),
            in_specs=[any_spec] * 11,
            out_specs=pl.BlockSpec(memory_space=pltpu.VMEM),
            scratch_shapes=[
                pltpu.VMEM((rows, d_model), BF16),
                pltpu.VMEM((1, rows), jnp.int32),
                pltpu.VMEM((2, layers, d_model), BF16),
                pltpu.VMEM(w_qkv.shape, BF16),
                pltpu.VMEM(w_out.shape, BF16),
                pltpu.VMEM(w_gate.shape, BF16),
                pltpu.VMEM(w_up.shape, BF16),
                pltpu.VMEM(w_down.shape, BF16),
                pltpu.VMEM((rows, head_dim, seq), BF16),
                pltpu.VMEM((rows, head_dim, seq), BF16),
                pltpu.VMEM((rows, 128), F32),
                pltpu.VMEM((rows, 128), F32),
                pltpu.VMEM((rows, 128), F32),
                pltpu.VMEM((4, rows, 128), F32),
                pltpu.VMEM((rows, 128), F32),
                pltpu.VMEM((rows, 128), F32),
                pltpu.VMEM((rows, w_out.shape[1]), BF16),
                pltpu.VMEM((rows, d_model), BF16),
                pltpu.VMEM((rows, w_down.shape[1]), BF16),
                pltpu.VMEM((rounds, 4, 2, rows, width), BF16),
                pltpu.VMEM((rounds, 2, 2, half, width), BF16),
                pltpu.VMEM((rounds, 2, half, width), BF16),
                pltpu.VMEM((rounds, rows, width), BF16),
                pltpu.VMEM((rounds, 2, 2, half, width), BF16),
                pltpu.VMEM((rounds, 2, half, width), F32),
                pltpu.VMEM((rounds, 2, half, width), F32),
                pltpu.VMEM((rounds, group, rows, width), BF16),
                sem((n_loads,)),
                sem((n_tiles,)),
                sem((n_tiles,)),
                sem((rounds * SLOTS,)),
                sem((rounds * SLOTS,)),
            ],
            compiler_params=pltpu.CompilerParams(
                collective_id=0, has_side_effects=True, vmem_limit_bytes=63 * 1024 * 1024),
            cost_estimate=pl.CostEstimate(flops=4 * 10**9, bytes_accessed=64 * 10**6, transcendentals=10**6),
            name="decode_layers",
        )(hidden, lengths.reshape(1, rows), keys, values, attn_norm, w_qkv, w_out, mlp_norm, w_gate, w_up, w_down)

    cache_spec = P(None, "dp", None, "tp", None)
    in_specs = (P("dp", None), P("dp"), cache_spec, cache_spec, P(), P(None, None, "tp", None),
                P(None, "tp", None), P(), P(None, None, "tp"), P(None, None, "tp"), P(None, "tp", None))
    return jax.shard_map(local_step, mesh=mesh, in_specs=in_specs, out_specs=P("dp", None), check_vma=False)
```

```python
import functools
import math

import jax
import jax.numpy as jnp
from jax import lax
from jax.experimental import pallas as pl
from jax.experimental.pallas import tpu as pltpu
from jax.sharding import PartitionSpec as P

ROPE_BASE = 10000.0
NORM_EPS = 1e-5
NEG = -1e30
TILE_ROWS = 16
VMEM_MIB = 56
F32 = jnp.float32
BF16 = jnp.bfloat16


def dot(a, b):
    return jnp.dot(a, b, preferred_element_type=F32)


def remote(src, dst, send_sem, recv_sem, device):
    return pltpu.make_async_remote_copy(
        src_ref=src, dst_ref=dst, send_sem=send_sem, recv_sem=recv_sem,
        device_id={"tp": device}, device_id_type=pl.DeviceIdType.MESH)


def kernel(group, layers, parts,
           hidden, lengths, k_hbm, v_hbm, attn_norm, w_qkv, w_out, mlp_norm, w_gate, w_up, w_down, out,
           x_in, len_in, gains, wq, wo, wg, wu, wd, kbuf, vbuf,
           cos_tab, sin_tab, len_tab, qq, kz, vz, attn, normed, act,
           block_out, block_in, xg,
           load_sem, k_sem, v_sem, rs_send, rs_recv, ag_send, ag_recv):
    rows, d_model = hidden.shape
    size = rows // parts
    width = d_model // group
    chips = group // 2
    me = lax.axis_index("tp")
    chip, core = me // 2, me % 2
    other = 1 - core
    sibling = chip * 2 + other
    right, left, far = (chip + 1) % chips, (chip + chips - 1) % chips, (chip + 2) % chips
    n_tiles = rows // TILE_ROWS
    seq = kbuf.shape[2]
    head_dim = kbuf.shape[1]
    ranges = [pl.ds(p * size, size) for p in range(parts)]

    loads = []

    def load(src, dst):
        copy = pltpu.make_async_copy(src, dst, load_sem.at[len(loads)])
        copy.start()
        loads.append(copy)
        return copy

    def load_cache(layer):
        for i in range(n_tiles):
            rng = pl.ds(i * TILE_ROWS, TILE_ROWS)
            pltpu.make_async_copy(k_hbm.at[layer, rng], kbuf.at[rng], k_sem.at[i]).start()
            pltpu.make_async_copy(v_hbm.at[layer, rng], vbuf.at[rng], v_sem.at[i]).start()

    ld_len = load(lengths, len_in)
    ld_x = load(hidden, x_in)
    ld_gain = [load(attn_norm, gains.at[0]), load(mlp_norm, gains.at[1])]
    ld_q = [load(w_qkv.at[0], wq.at[0])]
    load_cache(0)
    ld_o = [load(w_out.at[0], wo.at[0])]
    ld_g, ld_u, ld_d = [], [], []

    barrier = pltpu.get_barrier_semaphore()
    for step in range(1, group):
        pl.semaphore_signal(barrier, inc=1, device_id={"tp": (me + step) % group}, device_id_type=pl.DeviceIdType.MESH)
    pl.semaphore_wait(barrier, group - 1)

    ld_len.wait()
    len_row = jnp.broadcast_to(len_in[...].astype(F32), (rows, rows))
    len_tab[...] = len_row.T
    freq = lax.broadcasted_iota(jnp.int32, (head_dim // 2, rows), 0).astype(F32)
    angles = len_row[:head_dim // 2] * jnp.exp(freq * (-2.0 / head_dim * math.log(ROPE_BASE)))
    cosine, sine = jnp.cos(angles), jnp.sin(angles)
    cos_tab[...] = jnp.concatenate([cosine] * 4, axis=0).T
    sin_tab[...] = jnp.concatenate([-sine, sine, -sine, sine], axis=0).T

    def rms_norm(p, pieces, gain_row):
        total = jnp.zeros((size, 1), F32)
        for i in range(group):
            wide = pieces(i)
            total = total + jnp.sum(wide * wide, axis=1, keepdims=True)
        scale = lax.rsqrt(total / d_model + NORM_EPS)
        for i in range(group):
            cols = slice(i * width, (i + 1) * width)
            normed[ranges[p], cols] = (pieces(i) * scale * gain_row(cols)).astype(BF16)

    def attention(p, layer):
        part = ranges[p]
        fused = dot(normed[part, :], wq[layer]).astype(BF16).astype(F32)
        lane = lax.broadcasted_iota(jnp.int32, (size, 128), 1)
        first = lane % head_dim < head_dim // 2
        low = lane < head_dim
        cos, sin = cos_tab[part, :], sin_tab[part, :]

        def rope(x):
            swapped = jnp.where(first, pltpu.roll(x, 128 - head_dim // 2, 1), pltpu.roll(x, head_dim // 2, 1))
            return (x * cos + swapped * sin).astype(BF16).astype(F32)

        for pair in range(2):
            x = rope(fused[:, pair * 128:(pair + 1) * 128])
            swap = pltpu.roll(x, head_dim, 1)
            qq[2 * pair, part] = jnp.where(low, x, swap)
            qq[2 * pair + 1, part] = jnp.where(low, swap, x)
        kv = fused[:, 256:384]
        kz[part, :] = jnp.where(low, rope(kv), 0.0)
        vz[part, :] = pltpu.roll(kv, head_dim, 1)

        row16 = lax.broadcasted_iota(jnp.int32, (TILE_ROWS, 128), 0)
        high16 = lax.broadcasted_iota(jnp.int32, (TILE_ROWS, 128), 1) // head_dim
        pos = lax.broadcasted_iota(jnp.int32, (TILE_ROWS, seq), 1).astype(F32)
        col_row = lax.broadcasted_iota(jnp.int32, (head_dim, 4 * TILE_ROWS), 1) % TILE_ROWS

        def tile(i):
            rng = pl.ds(pl.multiple_of(i * TILE_ROWS, TILE_ROWS), TILE_ROWS)
            queries = [qq[g, rng, :] for g in range(4)]
            lhs = jnp.concatenate([
                jnp.concatenate([jnp.where(row16 == 2 * j + high16, q, 0.0).astype(BF16) for j in range(TILE_ROWS // 2)], axis=1)
                for q in queries], axis=0)
            pltpu.make_async_copy(k_hbm.at[layer, rng], kbuf.at[rng], k_sem.at[i]).wait()
            logits = dot(lhs, kbuf[rng].reshape(TILE_ROWS * head_dim, seq)) * head_dim ** -0.5
            live = pos < jnp.concatenate([len_tab[rng, :]] * (seq // 128), axis=1)
            keys = kz[rng, :]
            weights, sums, selfs = [], [], []
            for g in range(4):
                s = jnp.where(live, logits[g * TILE_ROWS:(g + 1) * TILE_ROWS], NEG)
                own = jnp.sum(queries[g] * keys, axis=1, keepdims=True) * head_dim ** -0.5
                peak = jnp.maximum(jnp.max(s, axis=1, keepdims=True), own)
                w = jnp.exp(s - peak).astype(BF16)
                w_own = jnp.exp(own - peak).astype(BF16).astype(F32)
                weights.append(w)
                selfs.append(w_own)
                sums.append(jnp.sum(w.astype(F32), axis=1, keepdims=True) + w_own)
            w_all = jnp.concatenate(weights, axis=0)
            pltpu.make_async_copy(v_hbm.at[layer, rng], vbuf.at[rng], v_sem.at[i]).wait()
            picked = lax.dot_general(vbuf[rng].reshape(TILE_ROWS * head_dim, seq), w_all, (((1,), (1,)), ((), ())),
                                     preferred_element_type=F32)
            numer = jnp.zeros((head_dim, 4 * TILE_ROWS), F32)
            for b in range(TILE_ROWS):
                numer = jnp.where(col_row == b, picked[b * head_dim:(b + 1) * head_dim], numer)
            numer = numer.T
            values = vz[rng, :][:, :head_dim]
            heads = [((numer[g * TILE_ROWS:(g + 1) * TILE_ROWS] + selfs[g] * values) / sums[g]).astype(BF16)
                     for g in range(4)]
            attn[rng, :] = jnp.concatenate(heads, axis=1)

        part_tiles = size // TILE_ROWS

        def pair_of_tiles(i, carry):
            tile(p * part_tiles + 2 * i)
            tile(p * part_tiles + 2 * i + 1)
            return carry

        lax.fori_loop(0, part_tiles // 2, pair_of_tiles, 0)

    opened = [[] for _ in range(parts)]

    def start(p, copy):
        copy.start()
        opened[p].append(copy)

    def drain(p):
        for copy in opened[p]:
            copy.wait_send()
        opened[p] = []

    def arrived(ref, sem):
        remote(ref, ref, rs_send.at[0, 0], sem, me).wait_recv()

    def scatter(p, lhs, weight):
        drain(p)
        for index, target in enumerate((far, right, left, chip)):
            cols = pl.ds(pl.multiple_of(target * 2 * width, 128), 2 * width)
            block = dot(lhs, weight[:, cols]).astype(BF16)
            block_out[p, index, 0] = block[:, :width]
            block_out[p, index, 1] = block[:, width:]
            if index < 3:
                for k in range(2):
                    start(p, remote(block_out.at[p, index, k], block_in.at[p, me], rs_send.at[p, 2 * index + k],
                                    rs_recv.at[p, me], target * 2 + k))
            else:
                start(p, remote(block_out.at[p, index, other], block_in.at[p, me], rs_send.at[p, 6], rs_recv.at[p, me],
                                sibling))

    def add_up(p, own_rows):
        total = own_rows.astype(F32) + block_out[p, 3, core].astype(F32)
        for source in (sibling, right * 2 + core, left * 2 + core, right * 2 + other, left * 2 + other,
                       far * 2 + core, far * 2 + other):
            arrived(block_in.at[p, source], rs_recv.at[p, source])
            total = total + block_in[p, source].astype(F32)
        xg[me, ranges[p]] = total.astype(BF16)
        mine = xg.at[me, ranges[p]]
        for index, target in enumerate((far * 2 + core, right * 2 + core, left * 2 + core, sibling)):
            start(p, remote(mine, mine, ag_send.at[p, index], ag_recv.at[p, me], target))

    def forward(p):
        for index, source in enumerate((right * 2 + core, left * 2 + core, far * 2 + core)):
            piece = xg.at[source, ranges[p]]
            arrived(piece, ag_recv.at[p, source])
            start(p, remote(piece, piece, ag_send.at[p, 4 + index], ag_recv.at[p, source], sibling))

    def gathered(p):
        for source in (sibling, right * 2 + other, left * 2 + other, far * 2 + other):
            arrived(xg.at[source, ranges[p]], ag_recv.at[p, source])

    def residual(p, stage):
        if stage == 0:
            return lambda i: x_in[ranges[p], i * width:(i + 1) * width].astype(F32)
        return lambda i: xg[i, ranges[p]].astype(F32)

    def compute(p, stage, hook):
        layer, which = stage // 2, stage % 2
        gain = lambda cols: gains[which, layer:layer + 1, cols].astype(F32)
        if stage > 0:
            gathered(p)
        elif p == 0:
            ld_x.wait()
            for copy in ld_gain:
                copy.wait()
        rms_norm(p, residual(p, stage), gain)
        if which == 0:
            if p == 0:
                ld_q[layer].wait()
            attention(p, layer)
            hook()
            if p == 0:
                ld_o[layer].wait()
            scatter(p, attn[ranges[p], :], wo.at[layer])
            return
        if p == 0:
            ld_g[layer].wait()
            ld_u[layer].wait()
        n = normed[ranges[p], :]
        for c in range(0, act.shape[1], 256):
            if c * 2 == act.shape[1]:
                hook()
            g = dot(n, wg[layer, :, c:c + 256]).astype(BF16).astype(F32)
            u = dot(n, wu[layer, :, c:c + 256]).astype(BF16).astype(F32)
            act[ranges[p], c:c + 256] = (g * jax.nn.sigmoid(g) * u).astype(BF16)
        if p == 0:
            ld_d[layer].wait()
        scatter(p, act[ranges[p], :], wd.at[layer])

    own_cols = pl.ds(pl.multiple_of(me * width, 128), width)
    for stage in range(2 * layers):
        for p in range(parts):
            behind = stage > 0 and p + 1 < parts
            compute(p, stage, (lambda q=p + 1: forward(q)) if behind else (lambda: None))
        if stage == 0:
            for layer in range(layers):
                ld_g.append(load(w_gate.at[layer], wg.at[layer]))
                ld_u.append(load(w_up.at[layer], wu.at[layer]))
                ld_d.append(load(w_down.at[layer], wd.at[layer]))
                if layer + 1 < layers:
                    ld_q.append(load(w_qkv.at[layer + 1], wq.at[layer + 1]))
                    load_cache(layer + 1)
                    ld_o.append(load(w_out.at[layer + 1], wo.at[layer + 1]))
        for p in range(parts):
            add_up(p, x_in[ranges[p], own_cols] if stage == 0 else xg[me, ranges[p]])
        forward(0)
    for p in range(parts):
        if p > 0:
            forward(p)
        gathered(p)
        for i in range(group):
            out[ranges[p], i * width:(i + 1) * width] = xg[i, ranges[p]]
        drain(p)


PARTS = 2


def solution(mesh):
    group = mesh.shape["tp"]

    def local_step(hidden, lengths, k_cache, v_cache, attn_norm, w_qkv, w_out, mlp_norm, w_gate, w_up, w_down):
        rows, d_model = hidden.shape
        layers, _, seq, _, head_dim = k_cache.shape
        width = d_model // group
        size = rows // PARTS
        fused_width = w_qkv.shape[-1]
        n_tiles = rows // TILE_ROWS
        keys = jnp.transpose(k_cache, (0, 1, 3, 4, 2)).reshape(layers, rows, head_dim, seq)
        values = jnp.transpose(v_cache, (0, 1, 3, 4, 2)).reshape(layers, rows, head_dim, seq)
        w_qkv = w_qkv.reshape(layers, d_model, fused_width)
        any_spec = pl.BlockSpec(memory_space=pl.ANY)
        sem = pltpu.SemaphoreType.DMA
        n_loads = 4 + 5 * layers
        return pl.pallas_call(
            functools.partial(kernel, group, layers, PARTS),
            out_shape=jax.ShapeDtypeStruct((rows, d_model), BF16),
            in_specs=[any_spec] * 11,
            out_specs=pl.BlockSpec(memory_space=pltpu.VMEM),
            scratch_shapes=[
                pltpu.VMEM((rows, d_model), BF16),
                pltpu.VMEM((1, rows), jnp.int32),
                pltpu.VMEM((2, layers, d_model), BF16),
                pltpu.VMEM(w_qkv.shape, BF16),
                pltpu.VMEM(w_out.shape, BF16),
                pltpu.VMEM(w_gate.shape, BF16),
                pltpu.VMEM(w_up.shape, BF16),
                pltpu.VMEM(w_down.shape, BF16),
                pltpu.VMEM((rows, head_dim, seq), BF16),
                pltpu.VMEM((rows, head_dim, seq), BF16),
                pltpu.VMEM((rows, 128), F32),
                pltpu.VMEM((rows, 128), F32),
                pltpu.VMEM((rows, 128), F32),
                pltpu.VMEM((4, rows, 128), F32),
                pltpu.VMEM((rows, 128), F32),
                pltpu.VMEM((rows, 128), F32),
                pltpu.VMEM((rows, w_out.shape[1]), BF16),
                pltpu.VMEM((rows, d_model), BF16),
                pltpu.VMEM((rows, w_down.shape[1]), BF16),
                pltpu.VMEM((PARTS, 4, 2, size, width), BF16),
                pltpu.VMEM((PARTS, group, size, width), BF16),
                pltpu.VMEM((group, rows, width), BF16),
                sem((n_loads,)),
                sem((n_tiles,)),
                sem((n_tiles,)),
                sem((PARTS, 7)),
                sem((PARTS, group)),
                sem((PARTS, 7)),
                sem((PARTS, group)),
            ],
            compiler_params=pltpu.CompilerParams(
                collective_id=0, has_side_effects=True, vmem_limit_bytes=VMEM_MIB * 1024 * 1024),
            cost_estimate=pl.CostEstimate(flops=4 * 10**9, bytes_accessed=64 * 10**6, transcendentals=10**6),
            name="decode_layers",
        )(hidden, lengths.reshape(1, rows), keys, values, attn_norm, w_qkv, w_out, mlp_norm, w_gate, w_up, w_down)

    cache_spec = P(None, "dp", None, "tp", None)
    in_specs = (P("dp", None), P("dp"), cache_spec, cache_spec, P(), P(None, None, "tp", None),
                P(None, "tp", None), P(), P(None, None, "tp"), P(None, None, "tp"), P(None, "tp", None))
    return jax.shard_map(local_step, mesh=mesh, in_specs=in_specs, out_specs=P("dp", None), check_vma=False)
```

```python
import functools
import math

import jax
import jax.numpy as jnp
from jax import lax
from jax.experimental import pallas as pl
from jax.experimental.pallas import tpu as pltpu
from jax.sharding import PartitionSpec as P

ROPE_BASE = 10000.0
NORM_EPS = 1e-5
NEG = -1e30
TILE_ROWS = 16
VMEM_MIB = 56
F32 = jnp.float32
BF16 = jnp.bfloat16


def dot(a, b):
    return jnp.dot(a, b, preferred_element_type=F32)


def remote(src, dst, send_sem, recv_sem, device):
    return pltpu.make_async_remote_copy(
        src_ref=src, dst_ref=dst, send_sem=send_sem, recv_sem=recv_sem,
        device_id={"tp": device}, device_id_type=pl.DeviceIdType.MESH)


def kernel(group, layers, parts, stages,
           hidden, lengths, k_hbm, v_hbm, attn_norm, w_qkv, w_out, mlp_norm, w_gate, w_up, w_down, out,
           x_in, len_in, gains, wq, wo, wg, wu, wd, kbuf, vbuf,
           cos_tab, sin_tab, len_tab, qq, kz, vz, attn, normed, act,
           block_out, block_in, xg,
           load_sem, k_sem, v_sem, rs_send, rs_recv, ag_send, ag_recv):
    rows, d_model = hidden.shape
    size = rows // parts
    width = d_model // group
    chips = group // 2
    me = lax.axis_index("tp")
    chip, core = me // 2, me % 2
    other = 1 - core
    sibling = chip * 2 + other
    right, left, far = (chip + 1) % chips, (chip + chips - 1) % chips, (chip + 2) % chips
    n_tiles = rows // TILE_ROWS
    seq = kbuf.shape[2]
    head_dim = kbuf.shape[1]
    ranges = [pl.ds(p * size, size) for p in range(parts)]

    loads = []

    def load(src, dst):
        copy = pltpu.make_async_copy(src, dst, load_sem.at[len(loads)])
        copy.start()
        loads.append(copy)
        return copy

    part_tiles = size // TILE_ROWS

    def cache_copies(layer, i):
        rng = pl.ds(i * TILE_ROWS, TILE_ROWS)
        return (pltpu.make_async_copy(k_hbm.at[layer, rng], kbuf.at[rng], k_sem.at[i]),
                pltpu.make_async_copy(v_hbm.at[layer, rng], vbuf.at[rng], v_sem.at[i]))

    def load_cache(layer, tiles):
        for i in tiles:
            for copy in cache_copies(layer, i):
                copy.start()

    ld_len = load(lengths, len_in)
    ld_x = load(hidden, x_in)
    ld_gain = [load(attn_norm, gains.at[0]), load(mlp_norm, gains.at[1])]
    ld_q = [load(w_qkv.at[0], wq.at[0])]
    load_cache(0, range(part_tiles))
    ld_o = [load(w_out.at[0], wo.at[0])]
    ld_g, ld_u, ld_d = [], [], []

    barrier = pltpu.get_barrier_semaphore()
    for step in range(1, group):
        pl.semaphore_signal(barrier, inc=1, device_id={"tp": (me + step) % group}, device_id_type=pl.DeviceIdType.MESH)

    ld_len.wait()
    len_row = jnp.broadcast_to(len_in[...].astype(F32), (rows, rows))
    len_tab[...] = len_row.T
    freq = lax.broadcasted_iota(jnp.int32, (head_dim // 2, rows), 0).astype(F32)
    angles = len_row[:head_dim // 2] * jnp.exp(freq * (-2.0 / head_dim * math.log(ROPE_BASE)))
    cosine, sine = jnp.cos(angles), jnp.sin(angles)
    cos_tab[...] = jnp.concatenate([cosine] * 4, axis=0).T
    sin_tab[...] = jnp.concatenate([-sine, sine, -sine, sine], axis=0).T

    def rms_norm(p, pieces, gain_row):
        total = jnp.zeros((size, 1), F32)
        for i in range(group):
            wide = pieces(i)
            total = total + jnp.sum(wide * wide, axis=1, keepdims=True)
        scale = lax.rsqrt(total / d_model + NORM_EPS)
        for i in range(group):
            cols = slice(i * width, (i + 1) * width)
            normed[ranges[p], cols] = (pieces(i) * scale * gain_row(cols)).astype(BF16)

    def attention(p, layer, hook):
        part = ranges[p]
        fused = dot(normed[part, :], wq[layer]).astype(BF16).astype(F32)
        lane = lax.broadcasted_iota(jnp.int32, (size, 128), 1)
        first = lane % head_dim < head_dim // 2
        low = lane < head_dim
        cos, sin = cos_tab[part, :], sin_tab[part, :]

        def rope(x):
            swapped = jnp.where(first, pltpu.roll(x, 128 - head_dim // 2, 1), pltpu.roll(x, head_dim // 2, 1))
            return (x * cos + swapped * sin).astype(BF16).astype(F32)

        for pair in range(2):
            x = rope(fused[:, pair * 128:(pair + 1) * 128])
            swap = pltpu.roll(x, head_dim, 1)
            qq[2 * pair, part] = jnp.where(low, x, swap)
            qq[2 * pair + 1, part] = jnp.where(low, swap, x)
        kv = fused[:, 256:384]
        kz[part, :] = jnp.where(low, rope(kv), 0.0)
        vz[part, :] = pltpu.roll(kv, head_dim, 1)

        row16 = lax.broadcasted_iota(jnp.int32, (TILE_ROWS, 128), 0)
        high16 = lax.broadcasted_iota(jnp.int32, (TILE_ROWS, 128), 1) // head_dim
        pos = lax.broadcasted_iota(jnp.int32, (TILE_ROWS, seq), 1).astype(F32)
        col_row = lax.broadcasted_iota(jnp.int32, (head_dim, 4 * TILE_ROWS), 1) % TILE_ROWS

        def tile(i):
            rng = pl.ds(i * TILE_ROWS, TILE_ROWS)
            keys_in, values_in = cache_copies(layer, i)
            queries = [qq[g, rng, :] for g in range(4)]
            lhs = jnp.concatenate([
                jnp.concatenate([jnp.where(row16 == 2 * j + high16, q, 0.0).astype(BF16) for j in range(TILE_ROWS // 2)], axis=1)
                for q in queries], axis=0)
            keys_in.wait()
            logits = dot(lhs, kbuf[rng].reshape(TILE_ROWS * head_dim, seq)) * head_dim ** -0.5
            live = pos < jnp.concatenate([len_tab[rng, :]] * (seq // 128), axis=1)
            keys = kz[rng, :]
            weights, sums, selfs = [], [], []
            for g in range(4):
                s = jnp.where(live, logits[g * TILE_ROWS:(g + 1) * TILE_ROWS], NEG)
                own = jnp.sum(queries[g] * keys, axis=1, keepdims=True) * head_dim ** -0.5
                peak = jnp.maximum(jnp.max(s, axis=1, keepdims=True), own)
                w = jnp.exp(s - peak).astype(BF16)
                w_own = jnp.exp(own - peak).astype(BF16).astype(F32)
                weights.append(w)
                selfs.append(w_own)
                sums.append(jnp.sum(w.astype(F32), axis=1, keepdims=True) + w_own)
            w_all = jnp.concatenate(weights, axis=0)
            values_in.wait()
            if layer == 0 and i + part_tiles < n_tiles:
                load_cache(0, [i + part_tiles])
            picked = lax.dot_general(vbuf[rng].reshape(TILE_ROWS * head_dim, seq), w_all, (((1,), (1,)), ((), ())),
                                     preferred_element_type=F32)
            numer = jnp.zeros((head_dim, 4 * TILE_ROWS), F32)
            for b in range(TILE_ROWS):
                numer = jnp.where(col_row == b, picked[b * head_dim:(b + 1) * head_dim], numer)
            numer = numer.T
            values = vz[rng, :][:, :head_dim]
            heads = [((numer[g * TILE_ROWS:(g + 1) * TILE_ROWS] + selfs[g] * values) / sums[g]).astype(BF16)
                     for g in range(4)]
            attn[rng, :] = jnp.concatenate(heads, axis=1)

        for t in range(part_tiles):
            if 2 * t == part_tiles:
                hook()
            tile(p * part_tiles + t)

    opened = [[] for _ in range(parts)]
    entered = []

    def start(p, copy):
        copy.start()
        opened[p].append(copy)

    def drain(p):
        for copy in opened[p]:
            copy.wait_send()
        opened[p] = []

    def arrived(ref, sem):
        remote(ref, ref, rs_send.at[0, 0], sem, me).wait_recv()

    def scatter(p, lhs, weight):
        drain(p)
        if not entered:
            pl.semaphore_wait(barrier, group - 1)
            entered.append(True)
        for index, target in enumerate((far, right, left, chip)):
            cols = pl.ds(pl.multiple_of(target * 2 * width, 128), 2 * width)
            block = dot(lhs, weight[:, cols]).astype(BF16)
            block_out[p, index, 0] = block[:, :width]
            block_out[p, index, 1] = block[:, width:]
            if index < 3:
                for k in range(2):
                    start(p, remote(block_out.at[p, index, k], block_in.at[p, me], rs_send.at[p, 2 * index + k],
                                    rs_recv.at[p, me], target * 2 + k))
            else:
                start(p, remote(block_out.at[p, index, other], block_in.at[p, me], rs_send.at[p, 6], rs_recv.at[p, me],
                                sibling))

    def add_up(p, own_rows):
        total = own_rows.astype(F32) + block_out[p, 3, core].astype(F32)
        for source in (sibling, right * 2 + core, left * 2 + core, right * 2 + other, left * 2 + other,
                       far * 2 + core, far * 2 + other):
            arrived(block_in.at[p, source], rs_recv.at[p, source])
            total = total + block_in[p, source].astype(F32)
        xg[me, ranges[p]] = total.astype(BF16)
        mine = xg.at[me, ranges[p]]
        for index, target in enumerate((far * 2 + core, right * 2 + core, left * 2 + core, sibling)):
            start(p, remote(mine, mine, ag_send.at[p, index], ag_recv.at[p, me], target))

    def forward(p):
        for index, source in enumerate((right * 2 + core, left * 2 + core, far * 2 + core)):
            piece = xg.at[source, ranges[p]]
            arrived(piece, ag_recv.at[p, source])
            start(p, remote(piece, piece, ag_send.at[p, 4 + index], ag_recv.at[p, source], sibling))

    def gathered(p):
        for source in (sibling, right * 2 + other, left * 2 + other, far * 2 + other):
            arrived(xg.at[source, ranges[p]], ag_recv.at[p, source])

    def residual(p, stage):
        if stage == 0:
            return lambda i: x_in[ranges[p], i * width:(i + 1) * width].astype(F32)
        return lambda i: xg[i, ranges[p]].astype(F32)

    def compute(p, stage, hook):
        layer, which = stage // 2, stage % 2
        gain = lambda cols: gains[which, layer:layer + 1, cols].astype(F32)
        if stage > 0:
            gathered(p)
        elif p == 0:
            ld_x.wait()
            for copy in ld_gain:
                copy.wait()
        rms_norm(p, residual(p, stage), gain)
        if which == 0:
            if p == 0:
                ld_q[layer].wait()
            attention(p, layer, hook)
            if p == 0:
                ld_o[layer].wait()
            scatter(p, attn[ranges[p], :], wo.at[layer])
            return
        if p == 0:
            ld_g[layer].wait()
            ld_u[layer].wait()
        n = normed[ranges[p], :]
        for c in range(0, act.shape[1], 256):
            if c * 2 == act.shape[1]:
                hook()
            g = dot(n, wg[layer, :, c:c + 256]).astype(BF16).astype(F32)
            u = dot(n, wu[layer, :, c:c + 256]).astype(BF16).astype(F32)
            act[ranges[p], c:c + 256] = (g * jax.nn.sigmoid(g) * u).astype(BF16)
        if p == 0:
            ld_d[layer].wait()
        scatter(p, act[ranges[p], :], wd.at[layer])

    own_cols = pl.ds(pl.multiple_of(me * width, 128), width)

    def finish(p, stage):
        add_up(p, x_in[ranges[p], own_cols] if stage == 0 else xg[me, ranges[p]])

    def load_weights(layer):
        ld_g.append(load(w_gate.at[layer], wg.at[layer]))
        ld_u.append(load(w_up.at[layer], wu.at[layer]))
        ld_d.append(load(w_down.at[layer], wd.at[layer]))

    ahead, behind = 0, 1
    for stage in range(stages):
        layer, following = stage // 2, stage + 1 < stages
        compute(ahead, stage, (lambda: finish(behind, stage - 1)) if stage > 0 else (lambda: None))
        if stage % 2 == 1 and following:
            ld_q.append(load(w_qkv.at[layer + 1], wq.at[layer + 1]))
            load_cache(layer + 1, range(n_tiles))
            ld_o.append(load(w_out.at[layer + 1], wo.at[layer + 1]))
        if stage > 0:
            forward(behind)
        if stage % 2 == 0 and stage > 0:
            load_weights(layer)
        compute(behind, stage, (lambda: finish(ahead, stage)) if stage > 0 else (lambda: None))
        if stage == 0:
            load_weights(layer)
            finish(ahead, stage)
        forward(ahead)
    finish(behind, stages - 1)

    def emit(p):
        gathered(p)
        for i in range(group):
            out[ranges[p], i * width:(i + 1) * width] = xg[i, ranges[p]]
        drain(p)

    emit(ahead)
    forward(behind)
    emit(behind)


PARTS = 2


def solution(mesh):
    group = mesh.shape["tp"]

    def local_step(hidden, lengths, k_cache, v_cache, attn_norm, w_qkv, w_out, mlp_norm, w_gate, w_up, w_down):
        rows, d_model = hidden.shape
        layers, _, seq, _, head_dim = k_cache.shape
        width = d_model // group
        size = rows // PARTS
        fused_width = w_qkv.shape[-1]
        n_tiles = rows // TILE_ROWS
        keys = jnp.transpose(k_cache, (0, 1, 3, 4, 2)).reshape(layers, rows, head_dim, seq)
        values = jnp.transpose(v_cache, (0, 1, 3, 4, 2)).reshape(layers, rows, head_dim, seq)
        w_qkv = w_qkv.reshape(layers, d_model, fused_width)
        any_spec = pl.BlockSpec(memory_space=pl.ANY)
        sem = pltpu.SemaphoreType.DMA
        n_loads = 4 + 5 * layers
        return pl.pallas_call(
            functools.partial(kernel, group, layers, PARTS, 2 * layers),
            out_shape=pltpu.VMEM((rows, d_model), BF16),
            in_specs=[any_spec] * 11,
            out_specs=pl.BlockSpec(memory_space=pltpu.VMEM),
            scratch_shapes=[
                pltpu.VMEM((rows, d_model), BF16),
                pltpu.VMEM((1, rows), jnp.int32),
                pltpu.VMEM((2, layers, d_model), BF16),
                pltpu.VMEM(w_qkv.shape, BF16),
                pltpu.VMEM(w_out.shape, BF16),
                pltpu.VMEM(w_gate.shape, BF16),
                pltpu.VMEM(w_up.shape, BF16),
                pltpu.VMEM(w_down.shape, BF16),
                pltpu.VMEM((rows, head_dim, seq), BF16),
                pltpu.VMEM((rows, head_dim, seq), BF16),
                pltpu.VMEM((rows, 128), F32),
                pltpu.VMEM((rows, 128), F32),
                pltpu.VMEM((rows, 128), F32),
                pltpu.VMEM((4, rows, 128), F32),
                pltpu.VMEM((rows, 128), F32),
                pltpu.VMEM((rows, 128), F32),
                pltpu.VMEM((rows, w_out.shape[1]), BF16),
                pltpu.VMEM((rows, d_model), BF16),
                pltpu.VMEM((rows, w_down.shape[1]), BF16),
                pltpu.VMEM((PARTS, 4, 2, size, width), BF16),
                pltpu.VMEM((PARTS, group, size, width), BF16),
                pltpu.VMEM((group, rows, width), BF16),
                sem((n_loads,)),
                sem((n_tiles,)),
                sem((n_tiles,)),
                sem((PARTS, 7)),
                sem((PARTS, group)),
                sem((PARTS, 7)),
                sem((PARTS, group)),
            ],
            compiler_params=pltpu.CompilerParams(
                collective_id=0, has_side_effects=True, vmem_limit_bytes=VMEM_MIB * 1024 * 1024),
            cost_estimate=pl.CostEstimate(flops=4 * 10**9, bytes_accessed=64 * 10**6, transcendentals=10**6),
            name="decode_layers",
        )(hidden, lengths.reshape(1, rows), keys, values, attn_norm, w_qkv, w_out, mlp_norm, w_gate, w_up, w_down)

    cache_spec = P(None, "dp", None, "tp", None)
    in_specs = (P("dp", None), P("dp"), cache_spec, cache_spec, P(), P(None, None, "tp", None),
                P(None, "tp", None), P(), P(None, None, "tp"), P(None, None, "tp"), P(None, "tp", None))
    return jax.shard_map(local_step, mesh=mesh, in_specs=in_specs, out_specs=P("dp", None), check_vma=False)
```

```python
import functools
import math

import jax
import jax.numpy as jnp
from jax import lax
from jax.experimental import pallas as pl
from jax.experimental.pallas import tpu as pltpu
from jax.sharding import PartitionSpec as P

ROPE_BASE = 10000.0
NORM_EPS = 1e-5
NEG = -1e30
TILE_ROWS = 16
VMEM_MIB = 56
F32 = jnp.float32
BF16 = jnp.bfloat16


def dot(a, b):
    return jnp.dot(a, b, preferred_element_type=F32)


def write_tables(len_in, len_tab, cos_tab, sin_tab, head_dim):
    rows = len_in.shape[1]
    len_row = jnp.broadcast_to(len_in[...].astype(F32), (rows, rows))
    len_tab[...] = len_row.T
    freq = lax.broadcasted_iota(jnp.int32, (head_dim // 2, rows), 0).astype(F32)
    angles = len_row[:head_dim // 2] * jnp.exp(freq * (-2.0 / head_dim * math.log(ROPE_BASE)))
    cosine, sine = jnp.cos(angles), jnp.sin(angles)
    cos_tab[...] = jnp.concatenate([cosine] * 4, axis=0).T
    sin_tab[...] = jnp.concatenate([-sine, sine, -sine, sine], axis=0).T


def write_normed(normed, part, group, pieces, gain_row):
    width = normed.shape[1] // group
    total = jnp.zeros((part.size, 1), F32)
    for i in range(group):
        wide = pieces(i)
        total = total + jnp.sum(wide * wide, axis=1, keepdims=True)
    scale = lax.rsqrt(total / normed.shape[1] + NORM_EPS)
    for i in range(group):
        cols = slice(i * width, (i + 1) * width)
        normed[part, cols] = (pieces(i) * scale * gain_row(cols)).astype(BF16)


def write_heads(fused, part, head_dim, cos_tab, sin_tab, qq, kz, vz):
    lane = lax.broadcasted_iota(jnp.int32, (part.size, 128), 1)
    first = lane % head_dim < head_dim // 2
    low = lane < head_dim
    cos, sin = cos_tab[part, :], sin_tab[part, :]

    def rope(x):
        swapped = jnp.where(first, pltpu.roll(x, 128 - head_dim // 2, 1), pltpu.roll(x, head_dim // 2, 1))
        return (x * cos + swapped * sin).astype(BF16).astype(F32)

    for pair in range(2):
        x = rope(fused[:, pair * 128:(pair + 1) * 128])
        swap = pltpu.roll(x, head_dim, 1)
        qq[2 * pair, part] = jnp.where(low, x, swap)
        qq[2 * pair + 1, part] = jnp.where(low, swap, x)
    kv = fused[:, 256:384]
    kz[part, :] = jnp.where(low, rope(kv), 0.0)
    vz[part, :] = pltpu.roll(kv, head_dim, 1)


def attend(rng, span, kbuf, vbuf, len_tab, qq, kz, vz, attn, keys_ready, values_ready):
    head_dim = kbuf.shape[1]
    row16 = lax.broadcasted_iota(jnp.int32, (TILE_ROWS, 128), 0)
    high16 = lax.broadcasted_iota(jnp.int32, (TILE_ROWS, 128), 1) // head_dim
    pos = lax.broadcasted_iota(jnp.int32, (TILE_ROWS, span), 1).astype(F32)
    col_row = lax.broadcasted_iota(jnp.int32, (head_dim, 4 * TILE_ROWS), 1) % TILE_ROWS
    queries = [qq[g, rng, :] for g in range(4)]
    lhs = jnp.concatenate([
        jnp.concatenate([jnp.where(row16 == 2 * j + high16, q, 0.0).astype(BF16) for j in range(TILE_ROWS // 2)], axis=1)
        for q in queries], axis=0)
    keys_ready()
    logits = dot(lhs, kbuf[rng, :, :span].reshape(TILE_ROWS * head_dim, span)) * head_dim ** -0.5
    live = pos < jnp.concatenate([len_tab[rng, :]] * (span // 128), axis=1)
    keys = kz[rng, :]
    weights, sums, selfs = [], [], []
    for g in range(4):
        s = jnp.where(live, logits[g * TILE_ROWS:(g + 1) * TILE_ROWS], NEG)
        own = jnp.sum(queries[g] * keys, axis=1, keepdims=True) * head_dim ** -0.5
        peak = jnp.maximum(jnp.max(s, axis=1, keepdims=True), own)
        w = jnp.exp(s - peak).astype(BF16)
        w_own = jnp.exp(own - peak).astype(BF16).astype(F32)
        weights.append(w)
        selfs.append(w_own)
        sums.append(jnp.sum(w.astype(F32), axis=1, keepdims=True) + w_own)
    w_all = jnp.concatenate(weights, axis=0)
    values_ready()
    picked = lax.dot_general(vbuf[rng, :, :span].reshape(TILE_ROWS * head_dim, span), w_all, (((1,), (1,)), ((), ())),
                             preferred_element_type=F32)
    numer = jnp.zeros((head_dim, 4 * TILE_ROWS), F32)
    for b in range(TILE_ROWS):
        numer = jnp.where(col_row == b, picked[b * head_dim:(b + 1) * head_dim], numer)
    numer = numer.T
    values = vz[rng, :][:, :head_dim]
    heads = [((numer[g * TILE_ROWS:(g + 1) * TILE_ROWS] + selfs[g] * values) / sums[g]).astype(BF16) for g in range(4)]
    attn[rng, :] = jnp.concatenate(heads, axis=1)


def first_kernel(group, hidden, lengths, len_flat, k_hbm, v_hbm, attn_norm, w_qkv, attn,
                 x_in, len_in, len_s, gains, wq, kbuf, vbuf, cos_tab, sin_tab, len_tab, qq, kz, vz, normed,
                 load_sem, k_sem, v_sem):
    rows, d_model = hidden.shape
    width = d_model // group
    head_dim, seq = kbuf.shape[1:]
    n_tiles = rows // TILE_ROWS
    everything = pl.ds(0, rows)
    waits = []

    def load(src, dst):
        copy = pltpu.make_async_copy(src, dst, load_sem.at[len(waits)])
        copy.start()
        waits.append(copy)

    def copies(rng, i, first):
        cols = pl.ds(0, 128) if first else pl.ds(128, seq - 128)
        slot = 0 if first else 1
        return (pltpu.make_async_copy(k_hbm.at[0, rng, :, cols], kbuf.at[rng, :, cols], k_sem.at[slot, i]),
                pltpu.make_async_copy(v_hbm.at[0, rng, :, cols], vbuf.at[rng, :, cols], v_sem.at[slot, i]))

    load(len_flat, len_s)
    load(lengths, len_in)
    load(hidden, x_in)
    load(attn_norm, gains)
    load(w_qkv.at[0], wq)
    for i in range(n_tiles):
        for copy in copies(pl.ds(i * TILE_ROWS, TILE_ROWS), i, True):
            copy.start()

    def tile_is_long(i):
        longest = len_s[i * TILE_ROWS]
        for b in range(1, TILE_ROWS):
            longest = jnp.maximum(longest, len_s[i * TILE_ROWS + b])
        return longest > 128

    waits[0].wait()
    for i in range(n_tiles):
        @pl.when(tile_is_long(i))
        def _():
            for copy in copies(pl.ds(i * TILE_ROWS, TILE_ROWS), i, False):
                copy.start()
    waits[1].wait()
    write_tables(len_in, len_tab, cos_tab, sin_tab, head_dim)
    waits[2].wait()
    waits[3].wait()
    write_normed(normed, everything, group, lambda i: x_in[:, i * width:(i + 1) * width].astype(F32),
                 lambda cols: gains[0:1, cols].astype(F32))
    waits[4].wait()
    fused = dot(normed[...], wq[...]).astype(BF16).astype(F32)
    write_heads(fused, everything, head_dim, cos_tab, sin_tab, qq, kz, vz)

    def tile(i, carry):
        rng = pl.ds(pl.multiple_of(i * TILE_ROWS, TILE_ROWS), TILE_ROWS)
        long = tile_is_long(i)
        keys_in, values_in = copies(rng, i, True)
        keys_in.wait()
        values_in.wait()

        @pl.when(long)
        def _():
            for copy in copies(rng, i, False):
                copy.wait()
            attend(rng, seq, kbuf, vbuf, len_tab, qq, kz, vz, attn, lambda: None, lambda: None)

        @pl.when(jnp.logical_not(long))
        def _():
            attend(rng, 128, kbuf, vbuf, len_tab, qq, kz, vz, attn, lambda: None, lambda: None)

        return carry

    lax.fori_loop(0, n_tiles, tile, 0)


def remote(src, dst, send_sem, recv_sem, device):
    return pltpu.make_async_remote_copy(
        src_ref=src, dst_ref=dst, send_sem=send_sem, recv_sem=recv_sem,
        device_id={"tp": device}, device_id_type=pl.DeviceIdType.MESH)


def kernel(group, layers, parts, stages,
           attn_first, hidden, lengths, k_hbm, v_hbm, attn_norm, w_qkv, w_out, mlp_norm, w_gate, w_up, w_down, out,
           x_in, len_in, gains, wq, wo, wg, wu, wd, kbuf, vbuf,
           cos_tab, sin_tab, len_tab, qq, kz, vz, attn, normed, act,
           block_out, block_in, xg,
           load_sem, k_sem, v_sem, rs_send, rs_recv, ag_send, ag_recv):
    rows, d_model = hidden.shape
    size = rows // parts
    width = d_model // group
    chips = group // 2
    me = lax.axis_index("tp")
    chip, core = me // 2, me % 2
    other = 1 - core
    sibling = chip * 2 + other
    right, left, far = (chip + 1) % chips, (chip + chips - 1) % chips, (chip + 2) % chips
    n_tiles = rows // TILE_ROWS
    seq = kbuf.shape[2]
    head_dim = kbuf.shape[1]
    ranges = [pl.ds(p * size, size) for p in range(parts)]

    loads = []

    def load(src, dst):
        copy = pltpu.make_async_copy(src, dst, load_sem.at[len(loads)])
        copy.start()
        loads.append(copy)
        return copy

    part_tiles = size // TILE_ROWS

    def cache_copies(layer, i):
        rng = pl.ds(i * TILE_ROWS, TILE_ROWS)
        return (pltpu.make_async_copy(k_hbm.at[layer, rng], kbuf.at[rng], k_sem.at[i]),
                pltpu.make_async_copy(v_hbm.at[layer, rng], vbuf.at[rng], v_sem.at[i]))

    def load_cache(layer, tiles):
        for i in tiles:
            for copy in cache_copies(layer, i):
                copy.start()

    ld_q, ld_o = [None], [load(w_out.at[0], wo.at[0])]
    ld_len = load(lengths, len_in)
    ld_x = load(hidden, x_in)
    ld_gain = [load(attn_norm, gains.at[0]), load(mlp_norm, gains.at[1])]
    ld_g, ld_u, ld_d = [], [], []

    barrier = pltpu.get_barrier_semaphore()
    for step in range(1, group):
        pl.semaphore_signal(barrier, inc=1, device_id={"tp": (me + step) % group}, device_id_type=pl.DeviceIdType.MESH)

    def attention(p, layer, hook):
        part = ranges[p]
        fused = dot(normed[part, :], wq[layer]).astype(BF16).astype(F32)
        write_heads(fused, part, head_dim, cos_tab, sin_tab, qq, kz, vz)
        for t in range(part_tiles):
            if 2 * t == part_tiles:
                hook()
            i = p * part_tiles + t
            keys_in, values_in = cache_copies(layer, i)
            attend(pl.ds(i * TILE_ROWS, TILE_ROWS), seq, kbuf, vbuf, len_tab, qq, kz, vz, attn, keys_in.wait, values_in.wait)

    opened = [[] for _ in range(parts)]
    entered = []

    def start(p, copy):
        copy.start()
        opened[p].append(copy)

    def drain(p):
        for copy in opened[p]:
            copy.wait_send()
        opened[p] = []

    def arrived(ref, sem):
        remote(ref, ref, rs_send.at[0, 0], sem, me).wait_recv()

    def scatter(p, lhs, weight):
        drain(p)
        if not entered:
            pl.semaphore_wait(barrier, group - 1)
            entered.append(True)
        for index, target in enumerate((far, right, left, chip)):
            cols = pl.ds(pl.multiple_of(target * 2 * width, 128), 2 * width)
            block = dot(lhs, weight[:, cols]).astype(BF16)
            block_out[p, index, 0] = block[:, :width]
            block_out[p, index, 1] = block[:, width:]
            if index < 3:
                for k in range(2):
                    start(p, remote(block_out.at[p, index, k], block_in.at[p, me], rs_send.at[p, 2 * index + k],
                                    rs_recv.at[p, me], target * 2 + k))
            else:
                start(p, remote(block_out.at[p, index, other], block_in.at[p, me], rs_send.at[p, 6], rs_recv.at[p, me],
                                sibling))

    def add_up(p, own_rows):
        total = own_rows.astype(F32) + block_out[p, 3, core].astype(F32)
        for source in (sibling, right * 2 + core, left * 2 + core, right * 2 + other, left * 2 + other,
                       far * 2 + core, far * 2 + other):
            arrived(block_in.at[p, source], rs_recv.at[p, source])
            total = total + block_in[p, source].astype(F32)
        xg[me, ranges[p]] = total.astype(BF16)
        mine = xg.at[me, ranges[p]]
        for index, target in enumerate((far * 2 + core, right * 2 + core, left * 2 + core, sibling)):
            start(p, remote(mine, mine, ag_send.at[p, index], ag_recv.at[p, me], target))

    def forward(p):
        for index, source in enumerate((right * 2 + core, left * 2 + core, far * 2 + core)):
            piece = xg.at[source, ranges[p]]
            arrived(piece, ag_recv.at[p, source])
            start(p, remote(piece, piece, ag_send.at[p, 4 + index], ag_recv.at[p, source], sibling))

    def gathered(p):
        for source in (sibling, right * 2 + other, left * 2 + other, far * 2 + other):
            arrived(xg.at[source, ranges[p]], ag_recv.at[p, source])

    def compute(p, stage, hook):
        layer, which = stage // 2, stage % 2
        gain = lambda cols: gains[which, layer:layer + 1, cols].astype(F32)
        if stage == 0:
            if p == 0:
                ld_o[0].wait()
            scatter(p, attn_first[ranges[p], :], wo.at[0])
            return
        gathered(p)
        write_normed(normed, ranges[p], group, lambda i: xg[i, ranges[p]].astype(F32), gain)
        if which == 0:
            if p == 0:
                ld_q[layer].wait()
            attention(p, layer, hook)
            if p == 0:
                ld_o[layer].wait()
            scatter(p, attn[ranges[p], :], wo.at[layer])
            return
        if p == 0:
            ld_g[layer].wait()
            ld_u[layer].wait()
        n = normed[ranges[p], :]
        for c in range(0, act.shape[1], 256):
            if c * 2 == act.shape[1]:
                hook()
            g = dot(n, wg[layer, :, c:c + 256]).astype(BF16).astype(F32)
            u = dot(n, wu[layer, :, c:c + 256]).astype(BF16).astype(F32)
            act[ranges[p], c:c + 256] = (g * jax.nn.sigmoid(g) * u).astype(BF16)
        if p == 0:
            ld_d[layer].wait()
        scatter(p, act[ranges[p], :], wd.at[layer])

    own_cols = pl.ds(pl.multiple_of(me * width, 128), width)

    def finish(p, stage):
        add_up(p, x_in[ranges[p], own_cols] if stage == 0 else xg[me, ranges[p]])

    def load_weights(layer):
        ld_g.append(load(w_gate.at[layer], wg.at[layer]))
        ld_u.append(load(w_up.at[layer], wu.at[layer]))
        ld_d.append(load(w_down.at[layer], wd.at[layer]))

    ahead, behind = 0, 1
    for stage in range(stages):
        layer, following = stage // 2, stage + 1 < stages
        compute(ahead, stage, (lambda: finish(behind, stage - 1)) if stage > 0 else (lambda: None))
        if stage % 2 == 1 and following:
            ld_q.append(load(w_qkv.at[layer + 1], wq.at[layer + 1]))
            load_cache(layer + 1, range(n_tiles))
            ld_o.append(load(w_out.at[layer + 1], wo.at[layer + 1]))
        if stage > 0:
            forward(behind)
        if stage % 2 == 0 and stage > 0:
            load_weights(layer)
        compute(behind, stage, (lambda: finish(ahead, stage)) if stage > 0 else (lambda: None))
        if stage == 0:
            load_weights(layer)
            ld_len.wait()
            write_tables(len_in, len_tab, cos_tab, sin_tab, head_dim)
            for copy in [ld_x] + ld_gain:
                copy.wait()
            finish(ahead, stage)
        forward(ahead)
    finish(behind, stages - 1)

    def emit(p):
        gathered(p)
        for i in range(group):
            out[ranges[p], i * width:(i + 1) * width] = xg[i, ranges[p]]
        drain(p)

    emit(ahead)
    forward(behind)
    emit(behind)


PARTS = 2


def solution(mesh):
    group = mesh.shape["tp"]

    def local_step(hidden, lengths, k_cache, v_cache, attn_norm, w_qkv, w_out, mlp_norm, w_gate, w_up, w_down):
        rows, d_model = hidden.shape
        layers, _, seq, _, head_dim = k_cache.shape
        width = d_model // group
        size = rows // PARTS
        fused_width = w_qkv.shape[-1]
        n_tiles = rows // TILE_ROWS
        keys = jnp.transpose(k_cache, (0, 1, 3, 4, 2)).reshape(layers, rows, head_dim, seq)
        values = jnp.transpose(v_cache, (0, 1, 3, 4, 2)).reshape(layers, rows, head_dim, seq)
        w_qkv = w_qkv.reshape(layers, d_model, fused_width)
        any_spec = pl.BlockSpec(memory_space=pl.ANY)
        sem = pltpu.SemaphoreType.DMA
        vmem = pltpu.VMEM
        attn_first = pl.pallas_call(
            functools.partial(first_kernel, group),
            out_shape=pltpu.VMEM((rows, w_out.shape[1]), BF16),
            in_specs=[any_spec] * 7,
            out_specs=pl.BlockSpec(memory_space=pltpu.VMEM),
            scratch_shapes=[
                vmem((rows, d_model), BF16),
                vmem((1, rows), jnp.int32),
                pltpu.SMEM((rows,), jnp.int32),
                vmem((layers, d_model), BF16),
                vmem((d_model, fused_width), BF16),
                vmem((rows, head_dim, seq), BF16),
                vmem((rows, head_dim, seq), BF16),
                vmem((rows, 128), F32),
                vmem((rows, 128), F32),
                vmem((rows, 128), F32),
                vmem((4, rows, 128), F32),
                vmem((rows, 128), F32),
                vmem((rows, 128), F32),
                vmem((rows, d_model), BF16),
                sem((5,)),
                sem((2, n_tiles)),
                sem((2, n_tiles)),
            ],
            compiler_params=pltpu.CompilerParams(vmem_limit_bytes=63 * 1024 * 1024),
            cost_estimate=pl.CostEstimate(flops=10**9, bytes_accessed=10**7, transcendentals=10**6),
            name="first_attention",
        )(hidden, lengths.reshape(1, rows), lengths, keys, values, attn_norm, w_qkv)
        attn_first = pltpu.with_memory_space_constraint(attn_first, pltpu.VMEM)
        n_loads = 4 + 5 * layers
        return pl.pallas_call(
            functools.partial(kernel, group, layers, PARTS, 2 * layers),
            out_shape=pltpu.VMEM((rows, d_model), BF16),
            in_specs=[pl.BlockSpec(memory_space=pltpu.VMEM)] + [any_spec] * 11,
            out_specs=pl.BlockSpec(memory_space=pltpu.VMEM),
            scratch_shapes=[
                pltpu.VMEM((rows, d_model), BF16),
                pltpu.VMEM((1, rows), jnp.int32),
                pltpu.VMEM((2, layers, d_model), BF16),
                pltpu.VMEM(w_qkv.shape, BF16),
                pltpu.VMEM(w_out.shape, BF16),
                pltpu.VMEM(w_gate.shape, BF16),
                pltpu.VMEM(w_up.shape, BF16),
                pltpu.VMEM(w_down.shape, BF16),
                pltpu.VMEM((rows, head_dim, seq), BF16),
                pltpu.VMEM((rows, head_dim, seq), BF16),
                pltpu.VMEM((rows, 128), F32),
                pltpu.VMEM((rows, 128), F32),
                pltpu.VMEM((rows, 128), F32),
                pltpu.VMEM((4, rows, 128), F32),
                pltpu.VMEM((rows, 128), F32),
                pltpu.VMEM((rows, 128), F32),
                pltpu.VMEM((rows, w_out.shape[1]), BF16),
                pltpu.VMEM((rows, d_model), BF16),
                pltpu.VMEM((rows, w_down.shape[1]), BF16),
                pltpu.VMEM((PARTS, 4, 2, size, width), BF16),
                pltpu.VMEM((PARTS, group, size, width), BF16),
                pltpu.VMEM((group, rows, width), BF16),
                sem((n_loads,)),
                sem((n_tiles,)),
                sem((n_tiles,)),
                sem((PARTS, 7)),
                sem((PARTS, group)),
                sem((PARTS, 7)),
                sem((PARTS, group)),
            ],
            compiler_params=pltpu.CompilerParams(
                collective_id=0, has_side_effects=True, vmem_limit_bytes=VMEM_MIB * 1024 * 1024),
            cost_estimate=pl.CostEstimate(flops=4 * 10**9, bytes_accessed=64 * 10**6, transcendentals=10**6),
            name="decode_layers",
        )(attn_first, hidden, lengths.reshape(1, rows), keys, values, attn_norm, w_qkv, w_out, mlp_norm, w_gate, w_up, w_down)

    cache_spec = P(None, "dp", None, "tp", None)
    in_specs = (P("dp", None), P("dp"), cache_spec, cache_spec, P(), P(None, None, "tp", None),
                P(None, "tp", None), P(), P(None, None, "tp"), P(None, None, "tp"), P(None, "tp", None))
    return jax.shard_map(local_step, mesh=mesh, in_specs=in_specs, out_specs=P("dp", None), check_vma=False)
```

```python
import functools
import math

import jax
import jax.numpy as jnp
from jax import lax
from jax.experimental import pallas as pl
from jax.experimental.pallas import tpu as pltpu
from jax.sharding import PartitionSpec as P

ROPE_BASE = 10000.0
NORM_EPS = 1e-5
NEG = -1e30
TILE_ROWS = 16
VMEM_MIB = 56
F32 = jnp.float32
BF16 = jnp.bfloat16


def dot(a, b):
    return jnp.dot(a, b, preferred_element_type=F32)


def write_tables(len_in, len_tab, cos_tab, sin_tab, head_dim):
    rows = len_in.shape[1]
    len_row = jnp.broadcast_to(len_in[...].astype(F32), (rows, rows))
    len_tab[...] = len_row.T
    freq = lax.broadcasted_iota(jnp.int32, (head_dim // 2, rows), 0).astype(F32)
    angles = len_row[:head_dim // 2] * jnp.exp(freq * (-2.0 / head_dim * math.log(ROPE_BASE)))
    cosine, sine = jnp.cos(angles), jnp.sin(angles)
    cos_tab[...] = jnp.concatenate([cosine] * 4, axis=0).T
    sin_tab[...] = jnp.concatenate([-sine, sine, -sine, sine], axis=0).T


def write_normed(normed, part, group, pieces, gain_row):
    width = normed.shape[1] // group
    total = jnp.zeros((part.size, 1), F32)
    for i in range(group):
        wide = pieces(i)
        total = total + jnp.sum(wide * wide, axis=1, keepdims=True)
    scale = lax.rsqrt(total / normed.shape[1] + NORM_EPS)
    for i in range(group):
        cols = slice(i * width, (i + 1) * width)
        normed[part, cols] = (pieces(i) * scale * gain_row(cols)).astype(BF16)


def write_heads(fused, part, head_dim, cos_tab, sin_tab, qq, kz, vz):
    lane = lax.broadcasted_iota(jnp.int32, (part.size, 128), 1)
    first = lane % head_dim < head_dim // 2
    low = lane < head_dim
    cos, sin = cos_tab[part, :], sin_tab[part, :]

    def rope(x):
        swapped = jnp.where(first, pltpu.roll(x, 128 - head_dim // 2, 1), pltpu.roll(x, head_dim // 2, 1))
        return (x * cos + swapped * sin).astype(BF16).astype(F32)

    for pair in range(2):
        x = rope(fused[:, pair * 128:(pair + 1) * 128])
        swap = pltpu.roll(x, head_dim, 1)
        qq[2 * pair, part] = jnp.where(low, x, swap)
        qq[2 * pair + 1, part] = jnp.where(low, swap, x)
    kv = fused[:, 256:384]
    kz[part, :] = jnp.where(low, rope(kv), 0.0)
    vz[part, :] = pltpu.roll(kv, head_dim, 1)


def attend(rng, span, kbuf, vbuf, len_tab, qq, kz, vz, attn):
    head_dim = kbuf.shape[1]
    row16 = lax.broadcasted_iota(jnp.int32, (TILE_ROWS, 128), 0)
    high16 = lax.broadcasted_iota(jnp.int32, (TILE_ROWS, 128), 1) // head_dim
    pos = lax.broadcasted_iota(jnp.int32, (TILE_ROWS, span), 1).astype(F32)
    col_row = lax.broadcasted_iota(jnp.int32, (head_dim, 4 * TILE_ROWS), 1) % TILE_ROWS
    queries = [qq[g, rng, :] for g in range(4)]
    lhs = jnp.concatenate([
        jnp.concatenate([jnp.where(row16 == 2 * j + high16, q, 0.0).astype(BF16) for j in range(TILE_ROWS // 2)], axis=1)
        for q in queries], axis=0)
    logits = dot(lhs, kbuf[rng, :, :span].reshape(TILE_ROWS * head_dim, span)) * head_dim ** -0.5
    live = pos < jnp.concatenate([len_tab[rng, :]] * (span // 128), axis=1)
    keys = kz[rng, :]
    weights, sums, selfs = [], [], []
    for g in range(4):
        s = jnp.where(live, logits[g * TILE_ROWS:(g + 1) * TILE_ROWS], NEG)
        own = jnp.sum(queries[g] * keys, axis=1, keepdims=True) * head_dim ** -0.5
        peak = jnp.maximum(jnp.max(s, axis=1, keepdims=True), own)
        w = jnp.exp(s - peak).astype(BF16)
        w_own = jnp.exp(own - peak).astype(BF16).astype(F32)
        weights.append(w)
        selfs.append(w_own)
        sums.append(jnp.sum(w.astype(F32), axis=1, keepdims=True) + w_own)
    w_all = jnp.concatenate(weights, axis=0)
    picked = lax.dot_general(vbuf[rng, :, :span].reshape(TILE_ROWS * head_dim, span), w_all, (((1,), (1,)), ((), ())),
                             preferred_element_type=F32)
    numer = jnp.zeros((head_dim, 4 * TILE_ROWS), F32)
    for b in range(TILE_ROWS):
        numer = jnp.where(col_row == b, picked[b * head_dim:(b + 1) * head_dim], numer)
    numer = numer.T
    values = vz[rng, :][:, :head_dim]
    heads = [((numer[g * TILE_ROWS:(g + 1) * TILE_ROWS] + selfs[g] * values) / sums[g]).astype(BF16) for g in range(4)]
    attn[rng, :] = jnp.concatenate(heads, axis=1)


def first_kernel(group, hidden, lengths, len_flat, k_hbm, v_hbm, attn_norm, w_qkv, w_out, blocks,
                 attn, x_in, len_in, len_s, gains, wq, wo, kbuf, vbuf, cos_tab, sin_tab, len_tab, qq, kz, vz, normed,
                 load_sem, k_sem, v_sem):
    rows, d_model = hidden.shape
    width = d_model // group
    head_dim, seq = kbuf.shape[1:]
    n_tiles = rows // TILE_ROWS
    everything = pl.ds(0, rows)
    waits = []

    def load(src, dst):
        copy = pltpu.make_async_copy(src, dst, load_sem.at[len(waits)])
        copy.start()
        waits.append(copy)

    def copies(rng, i, first):
        cols = pl.ds(0, 128) if first else pl.ds(128, seq - 128)
        slot = 0 if first else 1
        return (pltpu.make_async_copy(k_hbm.at[0, rng, :, cols], kbuf.at[rng, :, cols], k_sem.at[slot, i]),
                pltpu.make_async_copy(v_hbm.at[0, rng, :, cols], vbuf.at[rng, :, cols], v_sem.at[slot, i]))

    load(len_flat, len_s)
    load(lengths, len_in)
    load(hidden, x_in)
    load(attn_norm, gains)
    load(w_qkv.at[0], wq)
    for i in range(n_tiles):
        for copy in copies(pl.ds(i * TILE_ROWS, TILE_ROWS), i, True):
            copy.start()

    def tile_is_long(i):
        longest = len_s[i * TILE_ROWS]
        for b in range(1, TILE_ROWS):
            longest = jnp.maximum(longest, len_s[i * TILE_ROWS + b])
        return longest > 128

    waits[0].wait()
    for i in range(n_tiles):
        @pl.when(tile_is_long(i))
        def _():
            for copy in copies(pl.ds(i * TILE_ROWS, TILE_ROWS), i, False):
                copy.start()
    load(w_out.at[0], wo)
    waits[1].wait()
    write_tables(len_in, len_tab, cos_tab, sin_tab, head_dim)
    waits[2].wait()
    waits[3].wait()
    write_normed(normed, everything, group, lambda i: x_in[:, i * width:(i + 1) * width].astype(F32),
                 lambda cols: gains[0:1, cols].astype(F32))
    waits[4].wait()
    fused = dot(normed[...], wq[...]).astype(BF16).astype(F32)
    write_heads(fused, everything, head_dim, cos_tab, sin_tab, qq, kz, vz)

    for i in range(n_tiles):
        for copy in copies(pl.ds(i * TILE_ROWS, TILE_ROWS), i, True):
            copy.wait()
    for i in range(n_tiles):
        attend(pl.ds(i * TILE_ROWS, TILE_ROWS), 128, kbuf, vbuf, len_tab, qq, kz, vz, attn)

    def long_tile(i, carry):
        rng = pl.ds(pl.multiple_of(i * TILE_ROWS, TILE_ROWS), TILE_ROWS)

        @pl.when(tile_is_long(i))
        def _():
            for copy in copies(rng, i, False):
                copy.wait()
            attend(rng, seq, kbuf, vbuf, len_tab, qq, kz, vz, attn)

        return carry

    lax.fori_loop(0, n_tiles, long_tile, 0)
    waits[5].wait()
    parts, chips, _, size, _ = blocks.shape
    for p in range(parts):
        for target in range(chips):
            block = dot(attn[p * size:(p + 1) * size, :], wo[:, target * 2 * width:(target + 1) * 2 * width]).astype(BF16)
            blocks[p, target, 0] = block[:, :width]
            blocks[p, target, 1] = block[:, width:]


def remote(src, dst, send_sem, recv_sem, device):
    return pltpu.make_async_remote_copy(
        src_ref=src, dst_ref=dst, send_sem=send_sem, recv_sem=recv_sem,
        device_id={"tp": device}, device_id_type=pl.DeviceIdType.MESH)


def kernel(group, layers, parts, stages,
           blocks, hidden, lengths, k_hbm, v_hbm, attn_norm, w_qkv, w_out, mlp_norm, w_gate, w_up, w_down, out,
           x_in, len_in, gains, wq, wo, wg, wu, wd, kbuf, vbuf,
           cos_tab, sin_tab, len_tab, qq, kz, vz, attn, normed, act,
           block_out, block_in, xg,
           load_sem, k_sem, v_sem, rs_send, rs_recv, ag_send, ag_recv):
    rows, d_model = hidden.shape
    size = rows // parts
    width = d_model // group
    chips = group // 2
    me = lax.axis_index("tp")
    chip, core = me // 2, me % 2
    other = 1 - core
    sibling = chip * 2 + other
    right, left, far = (chip + 1) % chips, (chip + chips - 1) % chips, (chip + 2) % chips
    n_tiles = rows // TILE_ROWS
    seq = kbuf.shape[2]
    head_dim = kbuf.shape[1]
    ranges = [pl.ds(p * size, size) for p in range(parts)]

    loads = []

    def load(src, dst):
        copy = pltpu.make_async_copy(src, dst, load_sem.at[len(loads)])
        copy.start()
        loads.append(copy)
        return copy

    part_tiles = size // TILE_ROWS

    def cache_copies(layer, i):
        rng = pl.ds(i * TILE_ROWS, TILE_ROWS)
        return (pltpu.make_async_copy(k_hbm.at[layer, rng], kbuf.at[rng], k_sem.at[i]),
                pltpu.make_async_copy(v_hbm.at[layer, rng], vbuf.at[rng], v_sem.at[i]))

    def load_cache(layer, tiles):
        for i in tiles:
            for copy in cache_copies(layer, i):
                copy.start()

    ld_q, ld_o = [None], [None]
    ld_len = load(lengths, len_in)
    ld_x = load(hidden, x_in)
    ld_gain = [load(attn_norm, gains.at[0]), load(mlp_norm, gains.at[1])]
    ld_g, ld_u, ld_d = [], [], []

    barrier = pltpu.get_barrier_semaphore()
    for step in range(1, group):
        pl.semaphore_signal(barrier, inc=1, device_id={"tp": (me + step) % group}, device_id_type=pl.DeviceIdType.MESH)

    def attention(p, layer, hook):
        part = ranges[p]
        fused = dot(normed[part, :], wq[layer]).astype(BF16).astype(F32)
        write_heads(fused, part, head_dim, cos_tab, sin_tab, qq, kz, vz)
        tiles = range(p * part_tiles, (p + 1) * part_tiles)
        for i in tiles:
            for copy in cache_copies(layer, i):
                copy.wait()
        for i in tiles:
            if 2 * (i - tiles[0]) == part_tiles:
                hook()
            attend(pl.ds(i * TILE_ROWS, TILE_ROWS), seq, kbuf, vbuf, len_tab, qq, kz, vz, attn)

    opened = [[] for _ in range(parts)]

    def start(p, copy):
        copy.start()
        opened[p].append(copy)

    def drain(p):
        for copy in opened[p]:
            copy.wait_send()
        opened[p] = []

    def arrived(ref, sem):
        remote(ref, ref, rs_send.at[0, 0], sem, me).wait_recv()

    def send_blocks(p, index, target, pair):
        if index < 3:
            for k in range(2):
                start(p, remote(pair.at[k], block_in.at[p, me], rs_send.at[p, 2 * index + k], rs_recv.at[p, me],
                                target * 2 + k))
        else:
            start(p, remote(pair.at[other], block_in.at[p, me], rs_send.at[p, 6], rs_recv.at[p, me], sibling))

    def scatter(p, lhs, weight):
        drain(p)
        for index, target in enumerate((far, right, left, chip)):
            cols = pl.ds(pl.multiple_of(target * 2 * width, 128), 2 * width)
            block = dot(lhs, weight[:, cols]).astype(BF16)
            block_out[p, index, 0] = block[:, :width]
            block_out[p, index, 1] = block[:, width:]
            send_blocks(p, index, target, block_out.at[p, index])

    def add_up(p, own_rows, own_block):
        total = own_rows.astype(F32) + own_block.astype(F32)
        for source in (sibling, right * 2 + core, left * 2 + core, right * 2 + other, left * 2 + other,
                       far * 2 + core, far * 2 + other):
            arrived(block_in.at[p, source], rs_recv.at[p, source])
            total = total + block_in[p, source].astype(F32)
        xg[me, ranges[p]] = total.astype(BF16)
        mine = xg.at[me, ranges[p]]
        for index, target in enumerate((far * 2 + core, right * 2 + core, left * 2 + core, sibling)):
            start(p, remote(mine, mine, ag_send.at[p, index], ag_recv.at[p, me], target))

    def forward(p):
        for index, source in enumerate((right * 2 + core, left * 2 + core, far * 2 + core)):
            piece = xg.at[source, ranges[p]]
            arrived(piece, ag_recv.at[p, source])
            start(p, remote(piece, piece, ag_send.at[p, 4 + index], ag_recv.at[p, source], sibling))

    def gathered(p):
        for source in (sibling, right * 2 + other, left * 2 + other, far * 2 + other):
            arrived(xg.at[source, ranges[p]], ag_recv.at[p, source])

    def compute(p, stage, hook):
        layer, which = stage // 2, stage % 2
        gain = lambda cols: gains[which, layer:layer + 1, cols].astype(F32)
        if stage == 0:
            if p == 0:
                pl.semaphore_wait(barrier, group - 1)
            for index, target in enumerate((far, right, left, chip)):
                send_blocks(p, index, target, blocks.at[p, target])
            return
        gathered(p)
        write_normed(normed, ranges[p], group, lambda i: xg[i, ranges[p]].astype(F32), gain)
        if which == 0:
            if p == 0:
                ld_q[layer].wait()
            attention(p, layer, hook)
            if p == 0:
                ld_o[layer].wait()
            scatter(p, attn[ranges[p], :], wo.at[layer])
            return
        if p == 0:
            ld_g[layer].wait()
            ld_u[layer].wait()
        n = normed[ranges[p], :]
        for c in range(0, act.shape[1], 256):
            if c * 2 == act.shape[1]:
                hook()
            g = dot(n, wg[layer, :, c:c + 256]).astype(BF16).astype(F32)
            u = dot(n, wu[layer, :, c:c + 256]).astype(BF16).astype(F32)
            act[ranges[p], c:c + 256] = (g * jax.nn.sigmoid(g) * u).astype(BF16)
        if p == 0:
            ld_d[layer].wait()
        scatter(p, act[ranges[p], :], wd.at[layer])

    own_cols = pl.ds(pl.multiple_of(me * width, 128), width)

    def finish(p, stage):
        if stage == 0:
            add_up(p, x_in[ranges[p], own_cols], blocks[p, chip, core])
        else:
            add_up(p, xg[me, ranges[p]], block_out[p, 3, core])

    def load_weights(layer):
        ld_g.append(load(w_gate.at[layer], wg.at[layer]))
        ld_u.append(load(w_up.at[layer], wu.at[layer]))
        ld_d.append(load(w_down.at[layer], wd.at[layer]))

    ahead, behind = 0, 1
    for stage in range(stages):
        layer, following = stage // 2, stage + 1 < stages
        compute(ahead, stage, (lambda: finish(behind, stage - 1)) if stage > 0 else (lambda: None))
        if stage % 2 == 1 and following:
            ld_q.append(load(w_qkv.at[layer + 1], wq.at[layer + 1]))
            load_cache(layer + 1, range(n_tiles))
            ld_o.append(load(w_out.at[layer + 1], wo.at[layer + 1]))
        if stage > 0:
            forward(behind)
        if stage % 2 == 0 and stage > 0:
            load_weights(layer)
        compute(behind, stage, (lambda: finish(ahead, stage)) if stage > 0 else (lambda: None))
        if stage == 0:
            load_weights(layer)
            ld_len.wait()
            write_tables(len_in, len_tab, cos_tab, sin_tab, head_dim)
            for copy in [ld_x] + ld_gain:
                copy.wait()
            finish(ahead, stage)
        forward(ahead)
    finish(behind, stages - 1)

    def emit(p):
        gathered(p)
        for i in range(group):
            out[ranges[p], i * width:(i + 1) * width] = xg[i, ranges[p]]
        drain(p)

    emit(ahead)
    forward(behind)
    emit(behind)


PARTS = 2


def solution(mesh):
    group = mesh.shape["tp"]

    def local_step(hidden, lengths, k_cache, v_cache, attn_norm, w_qkv, w_out, mlp_norm, w_gate, w_up, w_down):
        rows, d_model = hidden.shape
        layers, _, seq, _, head_dim = k_cache.shape
        width = d_model // group
        size = rows // PARTS
        fused_width = w_qkv.shape[-1]
        n_tiles = rows // TILE_ROWS
        keys = jnp.transpose(k_cache, (0, 1, 3, 4, 2)).reshape(layers, rows, head_dim, seq)
        values = jnp.transpose(v_cache, (0, 1, 3, 4, 2)).reshape(layers, rows, head_dim, seq)
        w_qkv = w_qkv.reshape(layers, d_model, fused_width)
        any_spec = pl.BlockSpec(memory_space=pl.ANY)
        sem = pltpu.SemaphoreType.DMA
        vmem = pltpu.VMEM
        blocks = pl.pallas_call(
            functools.partial(first_kernel, group),
            out_shape=pltpu.VMEM((PARTS, group // 2, 2, size, width), BF16),
            in_specs=[any_spec] * 8,
            out_specs=pl.BlockSpec(memory_space=pltpu.VMEM),
            scratch_shapes=[
                vmem((rows, w_out.shape[1]), BF16),
                vmem((rows, d_model), BF16),
                vmem((1, rows), jnp.int32),
                pltpu.SMEM((rows,), jnp.int32),
                vmem((layers, d_model), BF16),
                vmem((d_model, fused_width), BF16),
                vmem(w_out.shape[1:], BF16),
                vmem((rows, head_dim, seq), BF16),
                vmem((rows, head_dim, seq), BF16),
                vmem((rows, 128), F32),
                vmem((rows, 128), F32),
                vmem((rows, 128), F32),
                vmem((4, rows, 128), F32),
                vmem((rows, 128), F32),
                vmem((rows, 128), F32),
                vmem((rows, d_model), BF16),
                sem((6,)),
                sem((2, n_tiles)),
                sem((2, n_tiles)),
            ],
            compiler_params=pltpu.CompilerParams(vmem_limit_bytes=63 * 1024 * 1024),
            cost_estimate=pl.CostEstimate(flops=10**9, bytes_accessed=10**7, transcendentals=10**6),
            name="first_attention",
        )(hidden, lengths.reshape(1, rows), lengths, keys, values, attn_norm, w_qkv, w_out)
        blocks = pltpu.with_memory_space_constraint(blocks, pltpu.VMEM)
        n_loads = 2 + 5 * layers + 1
        return pl.pallas_call(
            functools.partial(kernel, group, layers, PARTS, 2 * layers),
            out_shape=pltpu.VMEM((rows, d_model), BF16),
            in_specs=[pl.BlockSpec(memory_space=pltpu.VMEM)] + [any_spec] * 11,
            out_specs=pl.BlockSpec(memory_space=pltpu.VMEM),
            scratch_shapes=[
                pltpu.VMEM((rows, d_model), BF16),
                pltpu.VMEM((1, rows), jnp.int32),
                pltpu.VMEM((2, layers, d_model), BF16),
                pltpu.VMEM(w_qkv.shape, BF16),
                pltpu.VMEM(w_out.shape, BF16),
                pltpu.VMEM(w_gate.shape, BF16),
                pltpu.VMEM(w_up.shape, BF16),
                pltpu.VMEM(w_down.shape, BF16),
                pltpu.VMEM((rows, head_dim, seq), BF16),
                pltpu.VMEM((rows, head_dim, seq), BF16),
                pltpu.VMEM((rows, 128), F32),
                pltpu.VMEM((rows, 128), F32),
                pltpu.VMEM((rows, 128), F32),
                pltpu.VMEM((4, rows, 128), F32),
                pltpu.VMEM((rows, 128), F32),
                pltpu.VMEM((rows, 128), F32),
                pltpu.VMEM((rows, w_out.shape[1]), BF16),
                pltpu.VMEM((rows, d_model), BF16),
                pltpu.VMEM((rows, w_down.shape[1]), BF16),
                pltpu.VMEM((PARTS, 4, 2, size, width), BF16),
                pltpu.VMEM((PARTS, group, size, width), BF16),
                pltpu.VMEM((group, rows, width), BF16),
                sem((n_loads,)),
                sem((n_tiles,)),
                sem((n_tiles,)),
                sem((PARTS, 7)),
                sem((PARTS, group)),
                sem((PARTS, 7)),
                sem((PARTS, group)),
            ],
            compiler_params=pltpu.CompilerParams(
                collective_id=0, has_side_effects=True, vmem_limit_bytes=VMEM_MIB * 1024 * 1024),
            cost_estimate=pl.CostEstimate(flops=4 * 10**9, bytes_accessed=64 * 10**6, transcendentals=10**6),
            name="decode_layers",
        )(blocks, hidden, lengths.reshape(1, rows), keys, values, attn_norm, w_qkv, w_out, mlp_norm, w_gate, w_up, w_down)

    cache_spec = P(None, "dp", None, "tp", None)
    in_specs = (P("dp", None), P("dp"), cache_spec, cache_spec, P(), P(None, None, "tp", None),
                P(None, "tp", None), P(), P(None, None, "tp"), P(None, None, "tp"), P(None, "tp", None))
    return jax.shard_map(local_step, mesh=mesh, in_specs=in_specs, out_specs=P("dp", None), check_vma=False)
```

```python
import functools
import math

import jax
import jax.numpy as jnp
from jax import lax
from jax.experimental import pallas as pl
from jax.experimental.pallas import tpu as pltpu
from jax.sharding import PartitionSpec as P

ROPE_BASE = 10000.0
NORM_EPS = 1e-5
NEG = -1e30
TILE_ROWS = 16
VMEM_MIB = 56
F32 = jnp.float32
BF16 = jnp.bfloat16


def dot(a, b):
    return jnp.dot(a, b, preferred_element_type=F32)


def write_tables(len_in, len_tab, cos_tab, sin_tab, head_dim):
    rows = len_in.shape[1]
    len_row = jnp.broadcast_to(len_in[...].astype(F32), (rows, rows))
    len_tab[...] = len_row.T
    freq = lax.broadcasted_iota(jnp.int32, (head_dim // 2, rows), 0).astype(F32)
    angles = len_row[:head_dim // 2] * jnp.exp(freq * (-2.0 / head_dim * math.log(ROPE_BASE)))
    cosine, sine = jnp.cos(angles), jnp.sin(angles)
    cos_tab[...] = jnp.concatenate([cosine] * 4, axis=0).T
    sin_tab[...] = jnp.concatenate([-sine, sine, -sine, sine], axis=0).T


def write_normed(normed, part, group, pieces, gain_row, total=None):
    width = normed.shape[1] // group
    if total is None:
        total = jnp.zeros((part.size, 1), F32)
        for i in range(group):
            wide = pieces(i)
            total = total + jnp.sum(wide * wide, axis=1, keepdims=True)
    scale = lax.rsqrt(total / normed.shape[1] + NORM_EPS)
    for i in range(group):
        cols = slice(i * width, (i + 1) * width)
        normed[part, cols] = (pieces(i) * scale * gain_row(cols)).astype(BF16)


def write_heads(fused, part, head_dim, cos_tab, sin_tab, qq, kz, vz):
    lane = lax.broadcasted_iota(jnp.int32, (part.size, 128), 1)
    first = lane % head_dim < head_dim // 2
    low = lane < head_dim
    cos, sin = cos_tab[part, :], sin_tab[part, :]

    def rope(x):
        swapped = jnp.where(first, pltpu.roll(x, 128 - head_dim // 2, 1), pltpu.roll(x, head_dim // 2, 1))
        return (x * cos + swapped * sin).astype(BF16).astype(F32)

    for pair in range(2):
        x = rope(fused[:, pair * 128:(pair + 1) * 128])
        swap = pltpu.roll(x, head_dim, 1)
        qq[2 * pair, part] = jnp.where(low, x, swap)
        qq[2 * pair + 1, part] = jnp.where(low, swap, x)
    kv = fused[:, 256:384]
    kz[part, :] = jnp.where(low, rope(kv), 0.0)
    vz[part, :] = pltpu.roll(kv, head_dim, 1)


def attend(rng, span, kbuf, vbuf, len_tab, qq, kz, vz, attn):
    head_dim = kbuf.shape[1]
    row16 = lax.broadcasted_iota(jnp.int32, (TILE_ROWS, 128), 0)
    high16 = lax.broadcasted_iota(jnp.int32, (TILE_ROWS, 128), 1) // head_dim
    pos = lax.broadcasted_iota(jnp.int32, (TILE_ROWS, span), 1).astype(F32)
    col_row = lax.broadcasted_iota(jnp.int32, (head_dim, 4 * TILE_ROWS), 1) % TILE_ROWS
    queries = [qq[g, rng, :] for g in range(4)]
    lhs = jnp.concatenate([
        jnp.concatenate([jnp.where(row16 == 2 * j + high16, q, 0.0).astype(BF16) for j in range(TILE_ROWS // 2)], axis=1)
        for q in queries], axis=0)
    logits = dot(lhs, kbuf[rng, :, :span].reshape(TILE_ROWS * head_dim, span)) * head_dim ** -0.5
    live = pos < jnp.concatenate([len_tab[rng, :]] * (span // 128), axis=1)
    keys = kz[rng, :]
    weights, sums, selfs = [], [], []
    for g in range(4):
        s = jnp.where(live, logits[g * TILE_ROWS:(g + 1) * TILE_ROWS], NEG)
        own = jnp.sum(queries[g] * keys, axis=1, keepdims=True) * head_dim ** -0.5
        peak = jnp.maximum(jnp.max(s, axis=1, keepdims=True), own)
        w = jnp.exp(s - peak).astype(BF16)
        w_own = jnp.exp(own - peak).astype(BF16).astype(F32)
        weights.append(w)
        selfs.append(w_own)
        sums.append(jnp.sum(w.astype(F32), axis=1, keepdims=True) + w_own)
    w_all = jnp.concatenate(weights, axis=0)
    picked = lax.dot_general(vbuf[rng, :, :span].reshape(TILE_ROWS * head_dim, span), w_all, (((1,), (1,)), ((), ())),
                             preferred_element_type=F32)
    numer = jnp.zeros((head_dim, 4 * TILE_ROWS), F32)
    for b in range(TILE_ROWS):
        numer = jnp.where(col_row == b, picked[b * head_dim:(b + 1) * head_dim], numer)
    numer = numer.T
    values = vz[rng, :][:, :head_dim]
    heads = [((numer[g * TILE_ROWS:(g + 1) * TILE_ROWS] + selfs[g] * values) / sums[g]).astype(BF16) for g in range(4)]
    attn[rng, :] = jnp.concatenate(heads, axis=1)


def first_kernel(group, hidden, lengths, len_flat, k_hbm, v_hbm, attn_norm, w_qkv, w_out, blocks,
                 attn, x_in, len_in, len_s, gains, wq, wo, kbuf, vbuf, cos_tab, sin_tab, len_tab, qq, kz, vz, normed,
                 load_sem, k_sem, v_sem):
    rows, d_model = hidden.shape
    width = d_model // group
    head_dim, seq = kbuf.shape[1:]
    n_tiles = rows // TILE_ROWS
    everything = pl.ds(0, rows)
    waits = []

    def load(src, dst):
        copy = pltpu.make_async_copy(src, dst, load_sem.at[len(waits)])
        copy.start()
        waits.append(copy)

    def copies(rng, i, first):
        cols = pl.ds(0, 128) if first else pl.ds(128, seq - 128)
        slot = 0 if first else 1
        return (pltpu.make_async_copy(k_hbm.at[0, rng, :, cols], kbuf.at[rng, :, cols], k_sem.at[slot, i]),
                pltpu.make_async_copy(v_hbm.at[0, rng, :, cols], vbuf.at[rng, :, cols], v_sem.at[slot, i]))

    load(len_flat, len_s)
    load(lengths, len_in)
    load(hidden, x_in)
    load(attn_norm, gains)
    load(w_qkv.at[0], wq)
    for i in range(n_tiles):
        for copy in copies(pl.ds(i * TILE_ROWS, TILE_ROWS), i, True):
            copy.start()

    def tile_is_long(i):
        longest = len_s[i * TILE_ROWS]
        for b in range(1, TILE_ROWS):
            longest = jnp.maximum(longest, len_s[i * TILE_ROWS + b])
        return longest > 128

    waits[0].wait()
    for i in range(n_tiles):
        @pl.when(tile_is_long(i))
        def _():
            for copy in copies(pl.ds(i * TILE_ROWS, TILE_ROWS), i, False):
                copy.start()
    load(w_out.at[0], wo)
    waits[1].wait()
    write_tables(len_in, len_tab, cos_tab, sin_tab, head_dim)
    waits[2].wait()
    waits[3].wait()
    write_normed(normed, everything, group, lambda i: x_in[:, i * width:(i + 1) * width].astype(F32),
                 lambda cols: gains[0:1, cols].astype(F32))
    waits[4].wait()
    fused = dot(normed[...], wq[...]).astype(BF16).astype(F32)
    write_heads(fused, everything, head_dim, cos_tab, sin_tab, qq, kz, vz)

    for i in range(n_tiles):
        for copy in copies(pl.ds(i * TILE_ROWS, TILE_ROWS), i, True):
            copy.wait()
    for i in range(n_tiles):
        attend(pl.ds(i * TILE_ROWS, TILE_ROWS), 128, kbuf, vbuf, len_tab, qq, kz, vz, attn)

    def long_tile(i, carry):
        rng = pl.ds(pl.multiple_of(i * TILE_ROWS, TILE_ROWS), TILE_ROWS)

        @pl.when(tile_is_long(i))
        def _():
            for copy in copies(rng, i, False):
                copy.wait()
            attend(rng, seq, kbuf, vbuf, len_tab, qq, kz, vz, attn)

        return carry

    lax.fori_loop(0, n_tiles, long_tile, 0)
    waits[5].wait()
    parts, chips, _, size, _ = blocks.shape
    for p in range(parts):
        for target in range(chips):
            block = dot(attn[p * size:(p + 1) * size, :], wo[:, target * 2 * width:(target + 1) * 2 * width]).astype(BF16)
            blocks[p, target, 0] = block[:, :width]
            blocks[p, target, 1] = block[:, width:]


def remote(src, dst, send_sem, recv_sem, device):
    return pltpu.make_async_remote_copy(
        src_ref=src, dst_ref=dst, send_sem=send_sem, recv_sem=recv_sem,
        device_id={"tp": device}, device_id_type=pl.DeviceIdType.MESH)


def kernel(group, layers, parts, stages,
           blocks, hidden, lengths, k_hbm, v_hbm, attn_norm, w_qkv, w_out, mlp_norm, w_gate, w_up, w_down, out,
           x_in, len_in, gains, wq, wo, wg, wu, wd, kbuf, vbuf,
           cos_tab, sin_tab, len_tab, qq, kz, vz, attn, normed, act,
           block_out, block_in, xg,
           load_sem, k_sem, v_sem, rs_send, rs_recv, ag_send, ag_recv):
    rows, d_model = hidden.shape
    size = rows // parts
    width = d_model // group
    chips = group // 2
    me = lax.axis_index("tp")
    chip, core = me // 2, me % 2
    other = 1 - core
    sibling = chip * 2 + other
    right, left, far = (chip + 1) % chips, (chip + chips - 1) % chips, (chip + 2) % chips
    n_tiles = rows // TILE_ROWS
    seq = kbuf.shape[2]
    head_dim = kbuf.shape[1]
    ranges = [pl.ds(p * size, size) for p in range(parts)]

    loads = []

    def load(src, dst):
        copy = pltpu.make_async_copy(src, dst, load_sem.at[len(loads)])
        copy.start()
        loads.append(copy)
        return copy

    part_tiles = size // TILE_ROWS

    def cache_copies(layer, i):
        rng = pl.ds(i * TILE_ROWS, TILE_ROWS)
        return (pltpu.make_async_copy(k_hbm.at[layer, rng], kbuf.at[rng], k_sem.at[i]),
                pltpu.make_async_copy(v_hbm.at[layer, rng], vbuf.at[rng], v_sem.at[i]))

    def load_cache(layer, tiles):
        for i in tiles:
            for copy in cache_copies(layer, i):
                copy.start()

    ld_q, ld_o = [None], [None]
    ld_len = load(lengths, len_in)
    ld_x = load(hidden, x_in)
    ld_gain = [load(attn_norm, gains.at[0]), load(mlp_norm, gains.at[1])]
    ld_g, ld_u, ld_d = [], [], []

    barrier = pltpu.get_barrier_semaphore()
    for step in range(1, group):
        pl.semaphore_signal(barrier, inc=1, device_id={"tp": (me + step) % group}, device_id_type=pl.DeviceIdType.MESH)

    def attention(p, layer, hook):
        part = ranges[p]
        fused = dot(normed[part, :], wq[layer]).astype(BF16).astype(F32)
        write_heads(fused, part, head_dim, cos_tab, sin_tab, qq, kz, vz)
        tiles = range(p * part_tiles, (p + 1) * part_tiles)
        for i in tiles:
            for copy in cache_copies(layer, i):
                copy.wait()
        for i in tiles:
            if 2 * (i - tiles[0]) == part_tiles:
                hook()
            attend(pl.ds(i * TILE_ROWS, TILE_ROWS), seq, kbuf, vbuf, len_tab, qq, kz, vz, attn)

    opened = [[] for _ in range(parts)]

    def start(p, copy):
        copy.start()
        opened[p].append(copy)

    def drain(p):
        for copy in opened[p]:
            copy.wait_send()
        opened[p] = []

    def arrived(ref, sem):
        remote(ref, ref, rs_send.at[0, 0], sem, me).wait_recv()

    def send_blocks(p, index, target, pair):
        if index < 3:
            for k in range(2):
                start(p, remote(pair.at[k], block_in.at[p, me], rs_send.at[p, 2 * index + k], rs_recv.at[p, me],
                                target * 2 + k))
        else:
            start(p, remote(pair.at[other], block_in.at[p, me], rs_send.at[p, 6], rs_recv.at[p, me], sibling))

    def scatter(p, lhs, weight):
        drain(p)
        for index, target in enumerate((far, right, left, chip)):
            cols = pl.ds(pl.multiple_of(target * 2 * width, 128), 2 * width)
            block = dot(lhs, weight[:, cols]).astype(BF16)
            block_out[p, index, 0] = block[:, :width]
            block_out[p, index, 1] = block[:, width:]
            send_blocks(p, index, target, block_out.at[p, index])

    def add_up(p, own_rows, own_block):
        total = own_rows.astype(F32) + own_block.astype(F32)
        for source in (sibling, right * 2 + core, left * 2 + core, right * 2 + other, left * 2 + other,
                       far * 2 + core, far * 2 + other):
            arrived(block_in.at[p, source], rs_recv.at[p, source])
            total = total + block_in[p, source].astype(F32)
        xg[me, ranges[p]] = total.astype(BF16)
        mine = xg.at[me, ranges[p]]
        for index, target in enumerate((far * 2 + core, right * 2 + core, left * 2 + core, right * 2 + other,
                                        left * 2 + other, sibling)):
            start(p, remote(mine, mine, ag_send.at[p, index], ag_recv.at[p, me], target))

    def forward(p):
        source = far * 2 + core
        piece = xg.at[source, ranges[p]]
        arrived(piece, ag_recv.at[p, source])
        start(p, remote(piece, piece, ag_send.at[p, 6], ag_recv.at[p, source], sibling))

    def gathered(p, look=lambda source: None):
        look(me)
        for source in (sibling, right * 2 + core, left * 2 + core, right * 2 + other, left * 2 + other):
            arrived(xg.at[source, ranges[p]], ag_recv.at[p, source])
            look(source)
        look(far * 2 + core)
        source = far * 2 + other
        arrived(xg.at[source, ranges[p]], ag_recv.at[p, source])
        look(source)

    def compute(p, stage, hook):
        layer, which = stage // 2, stage % 2
        gain = lambda cols: gains[which, layer:layer + 1, cols].astype(F32)
        if stage == 0:
            if p == 0:
                pl.semaphore_wait(barrier, group - 1)
            for index, target in enumerate((far, right, left, chip)):
                send_blocks(p, index, target, blocks.at[p, target])
            return
        squares = []

        def look(source):
            wide = xg[source, ranges[p]].astype(F32)
            squares.append(jnp.sum(wide * wide, axis=1, keepdims=True))

        gathered(p, look)
        write_normed(normed, ranges[p], group, lambda i: xg[i, ranges[p]].astype(F32), gain, sum(squares))
        if which == 0:
            if p == 0:
                ld_q[layer].wait()
            attention(p, layer, hook)
            if p == 0:
                ld_o[layer].wait()
            scatter(p, attn[ranges[p], :], wo.at[layer])
            return
        if p == 0:
            ld_g[layer].wait()
            ld_u[layer].wait()
        n = normed[ranges[p], :]
        for c in range(0, act.shape[1], 256):
            if c * 2 == act.shape[1]:
                hook()
            g = dot(n, wg[layer, :, c:c + 256]).astype(BF16).astype(F32)
            u = dot(n, wu[layer, :, c:c + 256]).astype(BF16).astype(F32)
            act[ranges[p], c:c + 256] = (g * jax.nn.sigmoid(g) * u).astype(BF16)
        if p == 0:
            ld_d[layer].wait()
        scatter(p, act[ranges[p], :], wd.at[layer])

    own_cols = pl.ds(pl.multiple_of(me * width, 128), width)

    def finish(p, stage):
        if stage == 0:
            add_up(p, x_in[ranges[p], own_cols], blocks[p, chip, core])
        else:
            add_up(p, xg[me, ranges[p]], block_out[p, 3, core])

    def load_weights(layer):
        ld_g.append(load(w_gate.at[layer], wg.at[layer]))
        ld_u.append(load(w_up.at[layer], wu.at[layer]))
        ld_d.append(load(w_down.at[layer], wd.at[layer]))

    ahead, behind = 0, 1
    for stage in range(stages):
        layer, following = stage // 2, stage + 1 < stages
        compute(ahead, stage, (lambda: finish(behind, stage - 1)) if stage > 0 else (lambda: None))
        if stage % 2 == 1 and following:
            ld_q.append(load(w_qkv.at[layer + 1], wq.at[layer + 1]))
            load_cache(layer + 1, range(n_tiles))
            ld_o.append(load(w_out.at[layer + 1], wo.at[layer + 1]))
        if stage > 0:
            forward(behind)
        if stage % 2 == 0 and stage > 0:
            load_weights(layer)
        compute(behind, stage, (lambda: finish(ahead, stage)) if stage > 0 else (lambda: None))
        if stage == 0:
            load_weights(layer)
            ld_len.wait()
            write_tables(len_in, len_tab, cos_tab, sin_tab, head_dim)
            for copy in [ld_x] + ld_gain:
                copy.wait()
            finish(ahead, stage)
        forward(ahead)
    finish(behind, stages - 1)

    def emit(p):
        gathered(p)
        for i in range(group):
            out[ranges[p], i * width:(i + 1) * width] = xg[i, ranges[p]]
        drain(p)

    emit(ahead)
    forward(behind)
    emit(behind)


PARTS = 2


def solution(mesh):
    group = mesh.shape["tp"]

    def local_step(hidden, lengths, k_cache, v_cache, attn_norm, w_qkv, w_out, mlp_norm, w_gate, w_up, w_down):
        rows, d_model = hidden.shape
        layers, _, seq, _, head_dim = k_cache.shape
        width = d_model // group
        size = rows // PARTS
        fused_width = w_qkv.shape[-1]
        n_tiles = rows // TILE_ROWS
        keys = jnp.transpose(k_cache, (0, 1, 3, 4, 2)).reshape(layers, rows, head_dim, seq)
        values = jnp.transpose(v_cache, (0, 1, 3, 4, 2)).reshape(layers, rows, head_dim, seq)
        w_qkv = w_qkv.reshape(layers, d_model, fused_width)
        any_spec = pl.BlockSpec(memory_space=pl.ANY)
        sem = pltpu.SemaphoreType.DMA
        vmem = pltpu.VMEM
        blocks = pl.pallas_call(
            functools.partial(first_kernel, group),
            out_shape=pltpu.VMEM((PARTS, group // 2, 2, size, width), BF16),
            in_specs=[any_spec] * 8,
            out_specs=pl.BlockSpec(memory_space=pltpu.VMEM),
            scratch_shapes=[
                vmem((rows, w_out.shape[1]), BF16),
                vmem((rows, d_model), BF16),
                vmem((1, rows), jnp.int32),
                pltpu.SMEM((rows,), jnp.int32),
                vmem((layers, d_model), BF16),
                vmem((d_model, fused_width), BF16),
                vmem(w_out.shape[1:], BF16),
                vmem((rows, head_dim, seq), BF16),
                vmem((rows, head_dim, seq), BF16),
                vmem((rows, 128), F32),
                vmem((rows, 128), F32),
                vmem((rows, 128), F32),
                vmem((4, rows, 128), F32),
                vmem((rows, 128), F32),
                vmem((rows, 128), F32),
                vmem((rows, d_model), BF16),
                sem((6,)),
                sem((2, n_tiles)),
                sem((2, n_tiles)),
            ],
            compiler_params=pltpu.CompilerParams(vmem_limit_bytes=63 * 1024 * 1024),
            cost_estimate=pl.CostEstimate(flops=10**9, bytes_accessed=10**7, transcendentals=10**6),
            name="first_attention",
        )(hidden, lengths.reshape(1, rows), lengths, keys, values, attn_norm, w_qkv, w_out)
        blocks = pltpu.with_memory_space_constraint(blocks, pltpu.VMEM)
        n_loads = 2 + 5 * layers + 1
        return pl.pallas_call(
            functools.partial(kernel, group, layers, PARTS, 2 * layers),
            out_shape=pltpu.VMEM((rows, d_model), BF16),
            in_specs=[pl.BlockSpec(memory_space=pltpu.VMEM)] + [any_spec] * 11,
            out_specs=pl.BlockSpec(memory_space=pltpu.VMEM),
            scratch_shapes=[
                pltpu.VMEM((rows, d_model), BF16),
                pltpu.VMEM((1, rows), jnp.int32),
                pltpu.VMEM((2, layers, d_model), BF16),
                pltpu.VMEM(w_qkv.shape, BF16),
                pltpu.VMEM(w_out.shape, BF16),
                pltpu.VMEM(w_gate.shape, BF16),
                pltpu.VMEM(w_up.shape, BF16),
                pltpu.VMEM(w_down.shape, BF16),
                pltpu.VMEM((rows, head_dim, seq), BF16),
                pltpu.VMEM((rows, head_dim, seq), BF16),
                pltpu.VMEM((rows, 128), F32),
                pltpu.VMEM((rows, 128), F32),
                pltpu.VMEM((rows, 128), F32),
                pltpu.VMEM((4, rows, 128), F32),
                pltpu.VMEM((rows, 128), F32),
                pltpu.VMEM((rows, 128), F32),
                pltpu.VMEM((rows, w_out.shape[1]), BF16),
                pltpu.VMEM((rows, d_model), BF16),
                pltpu.VMEM((rows, w_down.shape[1]), BF16),
                pltpu.VMEM((PARTS, 4, 2, size, width), BF16),
                pltpu.VMEM((PARTS, group, size, width), BF16),
                pltpu.VMEM((group, rows, width), BF16),
                sem((n_loads,)),
                sem((n_tiles,)),
                sem((n_tiles,)),
                sem((PARTS, 7)),
                sem((PARTS, group)),
                sem((PARTS, 7)),
                sem((PARTS, group)),
            ],
            compiler_params=pltpu.CompilerParams(
                collective_id=0, has_side_effects=True, vmem_limit_bytes=VMEM_MIB * 1024 * 1024),
            cost_estimate=pl.CostEstimate(flops=4 * 10**9, bytes_accessed=64 * 10**6, transcendentals=10**6),
            name="decode_layers",
        )(blocks, hidden, lengths.reshape(1, rows), keys, values, attn_norm, w_qkv, w_out, mlp_norm, w_gate, w_up, w_down)

    cache_spec = P(None, "dp", None, "tp", None)
    in_specs = (P("dp", None), P("dp"), cache_spec, cache_spec, P(), P(None, None, "tp", None),
                P(None, "tp", None), P(), P(None, None, "tp"), P(None, None, "tp"), P(None, "tp", None))
    return jax.shard_map(local_step, mesh=mesh, in_specs=in_specs, out_specs=P("dp", None), check_vma=False)
```

```python
import functools
import math

import jax
import jax.numpy as jnp
from jax import lax
from jax.experimental import pallas as pl
from jax.experimental.pallas import tpu as pltpu
from jax.sharding import PartitionSpec as P

ROPE_BASE = 10000.0
NORM_EPS = 1e-5
NEG = -1e30
TILE_ROWS = 16
VMEM_MIB = 56
F32 = jnp.float32
BF16 = jnp.bfloat16


def dot(a, b):
    return jnp.dot(a, b, preferred_element_type=F32)


def write_tables(len_in, len_tab, cos_tab, sin_tab, head_dim):
    rows = len_in.shape[1]
    len_row = jnp.broadcast_to(len_in[...].astype(F32), (rows, rows))
    len_tab[...] = len_row.T
    freq = lax.broadcasted_iota(jnp.int32, (head_dim // 2, rows), 0).astype(F32)
    angles = len_row[:head_dim // 2] * jnp.exp(freq * (-2.0 / head_dim * math.log(ROPE_BASE)))
    cosine, sine = jnp.cos(angles), jnp.sin(angles)
    cos_tab[...] = jnp.concatenate([cosine] * 4, axis=0).T
    sin_tab[...] = jnp.concatenate([-sine, sine, -sine, sine], axis=0).T


def write_normed(normed, part, group, pieces, gain_row):
    width = normed.shape[1] // group
    folded = jnp.zeros((part.size, 128), F32)
    for i in range(group):
        wide = pieces(i)
        for c in range(0, width, 128):
            folded = folded + wide[:, c:c + 128] * wide[:, c:c + 128]
    scale = lax.rsqrt(jnp.sum(folded, axis=1, keepdims=True) / normed.shape[1] + NORM_EPS)
    for i in range(group):
        cols = slice(i * width, (i + 1) * width)
        normed[part, cols] = (pieces(i) * scale * gain_row(cols)).astype(BF16)


def write_heads(fused, part, head_dim, cos_tab, sin_tab, qq, kz, vz):
    lane = lax.broadcasted_iota(jnp.int32, (part.size, 128), 1)
    first = lane % head_dim < head_dim // 2
    low = lane < head_dim
    cos, sin = cos_tab[part, :], sin_tab[part, :]

    def rope(x):
        swapped = jnp.where(first, pltpu.roll(x, 128 - head_dim // 2, 1), pltpu.roll(x, head_dim // 2, 1))
        return (x * cos + swapped * sin).astype(BF16).astype(F32)

    for pair in range(2):
        x = rope(fused[:, pair * 128:(pair + 1) * 128])
        swap = pltpu.roll(x, head_dim, 1)
        qq[2 * pair, part] = jnp.where(low, x, swap)
        qq[2 * pair + 1, part] = jnp.where(low, swap, x)
    kv = fused[:, 256:384]
    kz[part, :] = jnp.where(low, rope(kv), 0.0)
    vz[part, :] = pltpu.roll(kv, head_dim, 1)


def attend(rng, span, kbuf, vbuf, len_tab, qq, kz, vz, attn):
    head_dim = kbuf.shape[1]
    row16 = lax.broadcasted_iota(jnp.int32, (TILE_ROWS, 128), 0)
    high16 = lax.broadcasted_iota(jnp.int32, (TILE_ROWS, 128), 1) // head_dim
    pos = lax.broadcasted_iota(jnp.int32, (TILE_ROWS, span), 1).astype(F32)
    col_row = lax.broadcasted_iota(jnp.int32, (head_dim, 4 * TILE_ROWS), 1) % TILE_ROWS
    queries = [qq[g, rng, :] for g in range(4)]
    lhs = jnp.concatenate([
        jnp.concatenate([jnp.where(row16 == 2 * j + high16, q, 0.0).astype(BF16) for j in range(TILE_ROWS // 2)], axis=1)
        for q in queries], axis=0)
    logits = dot(lhs, kbuf[rng, :, :span].reshape(TILE_ROWS * head_dim, span)) * head_dim ** -0.5
    live = pos < jnp.concatenate([len_tab[rng, :]] * (span // 128), axis=1)
    keys = kz[rng, :]
    weights, sums, selfs = [], [], []
    for g in range(4):
        s = jnp.where(live, logits[g * TILE_ROWS:(g + 1) * TILE_ROWS], NEG)
        own = jnp.sum(queries[g] * keys, axis=1, keepdims=True) * head_dim ** -0.5
        peak = jnp.maximum(jnp.max(s, axis=1, keepdims=True), own)
        w = jnp.exp(s - peak).astype(BF16)
        w_own = jnp.exp(own - peak).astype(BF16).astype(F32)
        weights.append(w)
        selfs.append(w_own)
        sums.append(jnp.sum(w.astype(F32), axis=1, keepdims=True) + w_own)
    w_all = jnp.concatenate(weights, axis=0)
    picked = lax.dot_general(vbuf[rng, :, :span].reshape(TILE_ROWS * head_dim, span), w_all, (((1,), (1,)), ((), ())),
                             preferred_element_type=F32)
    numer = jnp.zeros((head_dim, 4 * TILE_ROWS), F32)
    for b in range(TILE_ROWS):
        numer = jnp.where(col_row == b, picked[b * head_dim:(b + 1) * head_dim], numer)
    numer = numer.T
    values = vz[rng, :][:, :head_dim]
    heads = [((numer[g * TILE_ROWS:(g + 1) * TILE_ROWS] + selfs[g] * values) / sums[g]).astype(BF16) for g in range(4)]
    attn[rng, :] = jnp.concatenate(heads, axis=1)


def first_kernel(group, hidden, lengths, len_flat, k_hbm, v_hbm, attn_norm, w_qkv, w_out, blocks,
                 attn, x_in, len_in, len_s, gains, wq, wo, kbuf, vbuf, cos_tab, sin_tab, len_tab, qq, kz, vz, normed,
                 load_sem, k_sem, v_sem):
    rows, d_model = hidden.shape
    width = d_model // group
    head_dim, seq = kbuf.shape[1:]
    n_tiles = rows // TILE_ROWS
    everything = pl.ds(0, rows)
    waits = []

    def load(src, dst):
        copy = pltpu.make_async_copy(src, dst, load_sem.at[len(waits)])
        copy.start()
        waits.append(copy)

    def copies(rng, i, first):
        cols = pl.ds(0, 128) if first else pl.ds(128, seq - 128)
        slot = 0 if first else 1
        return (pltpu.make_async_copy(k_hbm.at[0, rng, :, cols], kbuf.at[rng, :, cols], k_sem.at[slot, i]),
                pltpu.make_async_copy(v_hbm.at[0, rng, :, cols], vbuf.at[rng, :, cols], v_sem.at[slot, i]))

    load(len_flat, len_s)
    load(lengths, len_in)
    load(hidden, x_in)
    load(attn_norm, gains)
    load(w_qkv.at[0], wq)
    for i in range(n_tiles):
        for copy in copies(pl.ds(i * TILE_ROWS, TILE_ROWS), i, True):
            copy.start()

    def tile_is_long(i):
        longest = len_s[i * TILE_ROWS]
        for b in range(1, TILE_ROWS):
            longest = jnp.maximum(longest, len_s[i * TILE_ROWS + b])
        return longest > 128

    waits[0].wait()
    for i in range(n_tiles):
        @pl.when(tile_is_long(i))
        def _():
            for copy in copies(pl.ds(i * TILE_ROWS, TILE_ROWS), i, False):
                copy.start()
    load(w_out.at[0], wo)
    waits[1].wait()
    write_tables(len_in, len_tab, cos_tab, sin_tab, head_dim)
    waits[2].wait()
    waits[3].wait()
    write_normed(normed, everything, group, lambda i: x_in[:, i * width:(i + 1) * width].astype(F32),
                 lambda cols: gains[0:1, cols].astype(F32))
    waits[4].wait()
    fused = dot(normed[...], wq[...]).astype(BF16).astype(F32)
    write_heads(fused, everything, head_dim, cos_tab, sin_tab, qq, kz, vz)

    for i in range(n_tiles):
        for copy in copies(pl.ds(i * TILE_ROWS, TILE_ROWS), i, True):
            copy.wait()
    for i in range(n_tiles):
        attend(pl.ds(i * TILE_ROWS, TILE_ROWS), 128, kbuf, vbuf, len_tab, qq, kz, vz, attn)

    def long_tile(i, carry):
        rng = pl.ds(pl.multiple_of(i * TILE_ROWS, TILE_ROWS), TILE_ROWS)

        @pl.when(tile_is_long(i))
        def _():
            for copy in copies(rng, i, False):
                copy.wait()
            attend(rng, seq, kbuf, vbuf, len_tab, qq, kz, vz, attn)

        return carry

    lax.fori_loop(0, n_tiles, long_tile, 0)
    waits[5].wait()
    parts, chips, _, size, _ = blocks.shape
    for p in range(parts):
        for target in range(chips):
            block = dot(attn[p * size:(p + 1) * size, :], wo[:, target * 2 * width:(target + 1) * 2 * width]).astype(BF16)
            blocks[p, target, 0] = block[:, :width]
            blocks[p, target, 1] = block[:, width:]


def remote(src, dst, send_sem, recv_sem, device):
    return pltpu.make_async_remote_copy(
        src_ref=src, dst_ref=dst, send_sem=send_sem, recv_sem=recv_sem,
        device_id={"tp": device}, device_id_type=pl.DeviceIdType.MESH)


def kernel(group, layers, parts, stages,
           blocks, hidden, lengths, k_hbm, v_hbm, attn_norm, w_qkv, w_out, mlp_norm, w_gate, w_up, w_down, out,
           x_in, len_in, gains, wq, wo, wg, wu, wd, kbuf, vbuf,
           cos_tab, sin_tab, len_tab, qq, kz, vz, attn, normed, act,
           block_out, block_in, xg,
           load_sem, k_sem, v_sem, rs_send, rs_recv, ag_send, ag_recv):
    rows, d_model = hidden.shape
    size = rows // parts
    width = d_model // group
    chips = group // 2
    me = lax.axis_index("tp")
    chip, core = me // 2, me % 2
    other = 1 - core
    sibling = chip * 2 + other
    right, left, far = (chip + 1) % chips, (chip + chips - 1) % chips, (chip + 2) % chips
    n_tiles = rows // TILE_ROWS
    seq = kbuf.shape[2]
    head_dim = kbuf.shape[1]
    ranges = [pl.ds(p * size, size) for p in range(parts)]

    loads = []

    def load(src, dst):
        copy = pltpu.make_async_copy(src, dst, load_sem.at[len(loads)])
        copy.start()
        loads.append(copy)
        return copy

    part_tiles = size // TILE_ROWS

    def cache_copies(layer, i):
        rng = pl.ds(i * TILE_ROWS, TILE_ROWS)
        return (pltpu.make_async_copy(k_hbm.at[layer, rng], kbuf.at[rng], k_sem.at[i]),
                pltpu.make_async_copy(v_hbm.at[layer, rng], vbuf.at[rng], v_sem.at[i]))

    def load_cache(layer, tiles):
        for i in tiles:
            for copy in cache_copies(layer, i):
                copy.start()

    ld_q, ld_o = [None], [None]
    ld_len = load(lengths, len_in)
    ld_x = load(hidden, x_in)
    ld_gain = [load(attn_norm, gains.at[0]), load(mlp_norm, gains.at[1])]
    ld_g, ld_u, ld_d = [], [], []

    barrier = pltpu.get_barrier_semaphore()
    for step in range(1, group):
        pl.semaphore_signal(barrier, inc=1, device_id={"tp": (me + step) % group}, device_id_type=pl.DeviceIdType.MESH)

    def attention(p, layer, hook):
        part = ranges[p]
        fused = dot(normed[part, :], wq[layer]).astype(BF16).astype(F32)
        write_heads(fused, part, head_dim, cos_tab, sin_tab, qq, kz, vz)
        tiles = range(p * part_tiles, (p + 1) * part_tiles)
        for i in tiles:
            for copy in cache_copies(layer, i):
                copy.wait()
        for i in tiles:
            if 2 * (i - tiles[0]) == part_tiles:
                hook()
            attend(pl.ds(i * TILE_ROWS, TILE_ROWS), seq, kbuf, vbuf, len_tab, qq, kz, vz, attn)

    opened = [[] for _ in range(parts)]

    def start(p, copy):
        copy.start()
        opened[p].append(copy)

    def drain(p):
        for copy in opened[p]:
            copy.wait_send()
        opened[p] = []

    def arrived(ref, sem):
        remote(ref, ref, rs_send.at[0, 0], sem, me).wait_recv()

    def send_blocks(p, index, target, pair):
        if index < 3:
            for k in range(2):
                start(p, remote(pair.at[k], block_in.at[p, me], rs_send.at[p, 2 * index + k], rs_recv.at[p, me],
                                target * 2 + k))
        else:
            start(p, remote(pair.at[other], block_in.at[p, me], rs_send.at[p, 6], rs_recv.at[p, me], sibling))

    def scatter(p, lhs, weight):
        drain(p)
        for index, target in enumerate((far, right, left, chip)):
            cols = pl.ds(pl.multiple_of(target * 2 * width, 128), 2 * width)
            block = dot(lhs, weight[:, cols]).astype(BF16)
            block_out[p, index, 0] = block[:, :width]
            block_out[p, index, 1] = block[:, width:]
            send_blocks(p, index, target, block_out.at[p, index])

    def add_up(p, own_rows, own_block):
        total = own_rows.astype(F32) + own_block.astype(F32)
        for source in (sibling, right * 2 + core, left * 2 + core, right * 2 + other, left * 2 + other,
                       far * 2 + core, far * 2 + other):
            arrived(block_in.at[p, source], rs_recv.at[p, source])
            total = total + block_in[p, source].astype(F32)
        xg[me, ranges[p]] = total.astype(BF16)
        mine = xg.at[me, ranges[p]]
        for index, target in enumerate((far * 2 + core, right * 2 + core, left * 2 + core, sibling)):
            start(p, remote(mine, mine, ag_send.at[p, index], ag_recv.at[p, me], target))

    def forward(p):
        for index, source in enumerate((right * 2 + core, left * 2 + core, far * 2 + core)):
            piece = xg.at[source, ranges[p]]
            arrived(piece, ag_recv.at[p, source])
            start(p, remote(piece, piece, ag_send.at[p, 4 + index], ag_recv.at[p, source], sibling))

    def gathered(p):
        for source in (sibling, right * 2 + other, left * 2 + other, far * 2 + other):
            arrived(xg.at[source, ranges[p]], ag_recv.at[p, source])

    def compute(p, stage, hook):
        layer, which = stage // 2, stage % 2
        gain = lambda cols: gains[which, layer:layer + 1, cols].astype(F32)
        if stage == 0:
            if p == 0:
                pl.semaphore_wait(barrier, group - 1)
            for index, target in enumerate((far, right, left, chip)):
                send_blocks(p, index, target, blocks.at[p, target])
            return
        gathered(p)
        write_normed(normed, ranges[p], group, lambda i: xg[i, ranges[p]].astype(F32), gain)
        if which == 0:
            if p == 0:
                ld_q[layer].wait()
            attention(p, layer, hook)
            if p == 0:
                ld_o[layer].wait()
            scatter(p, attn[ranges[p], :], wo.at[layer])
            return
        if p == 0:
            ld_g[layer].wait()
            ld_u[layer].wait()
        n = normed[ranges[p], :]
        for c in range(0, act.shape[1], 256):
            if c * 2 == act.shape[1]:
                hook()
            g = dot(n, wg[layer, :, c:c + 256]).astype(BF16).astype(F32)
            u = dot(n, wu[layer, :, c:c + 256]).astype(BF16).astype(F32)
            act[ranges[p], c:c + 256] = (g * jax.nn.sigmoid(g) * u).astype(BF16)
        if p == 0:
            ld_d[layer].wait()
        scatter(p, act[ranges[p], :], wd.at[layer])

    own_cols = pl.ds(pl.multiple_of(me * width, 128), width)

    def finish(p, stage):
        if stage == 0:
            add_up(p, x_in[ranges[p], own_cols], blocks[p, chip, core])
        else:
            add_up(p, xg[me, ranges[p]], block_out[p, 3, core])

    def load_weights(layer):
        ld_g.append(load(w_gate.at[layer], wg.at[layer]))
        ld_u.append(load(w_up.at[layer], wu.at[layer]))
        ld_d.append(load(w_down.at[layer], wd.at[layer]))

    ahead, behind = 0, 1
    for stage in range(stages):
        layer, following = stage // 2, stage + 1 < stages
        compute(ahead, stage, (lambda: finish(behind, stage - 1)) if stage > 0 else (lambda: None))
        if stage % 2 == 1 and following:
            ld_q.append(load(w_qkv.at[layer + 1], wq.at[layer + 1]))
            load_cache(layer + 1, range(n_tiles))
            ld_o.append(load(w_out.at[layer + 1], wo.at[layer + 1]))
        if stage > 0:
            forward(behind)
        if stage % 2 == 0 and stage > 0:
            load_weights(layer)
        compute(behind, stage, (lambda: finish(ahead, stage)) if stage > 0 else (lambda: None))
        if stage == 0:
            load_weights(layer)
            ld_len.wait()
            write_tables(len_in, len_tab, cos_tab, sin_tab, head_dim)
            for copy in [ld_x] + ld_gain:
                copy.wait()
            finish(ahead, stage)
        forward(ahead)
    finish(behind, stages - 1)

    def emit(p):
        gathered(p)
        for i in range(group):
            out[ranges[p], i * width:(i + 1) * width] = xg[i, ranges[p]]
        drain(p)

    emit(ahead)
    forward(behind)
    emit(behind)


PARTS = 2


def solution(mesh):
    group = mesh.shape["tp"]

    def local_step(hidden, lengths, k_cache, v_cache, attn_norm, w_qkv, w_out, mlp_norm, w_gate, w_up, w_down):
        rows, d_model = hidden.shape
        layers, _, seq, _, head_dim = k_cache.shape
        width = d_model // group
        size = rows // PARTS
        fused_width = w_qkv.shape[-1]
        n_tiles = rows // TILE_ROWS
        keys = jnp.transpose(k_cache, (0, 1, 3, 4, 2)).reshape(layers, rows, head_dim, seq)
        values = jnp.transpose(v_cache, (0, 1, 3, 4, 2)).reshape(layers, rows, head_dim, seq)
        w_qkv = w_qkv.reshape(layers, d_model, fused_width)
        any_spec = pl.BlockSpec(memory_space=pl.ANY)
        sem = pltpu.SemaphoreType.DMA
        vmem = pltpu.VMEM
        blocks = pl.pallas_call(
            functools.partial(first_kernel, group),
            out_shape=pltpu.VMEM((PARTS, group // 2, 2, size, width), BF16),
            in_specs=[any_spec] * 8,
            out_specs=pl.BlockSpec(memory_space=pltpu.VMEM),
            scratch_shapes=[
                vmem((rows, w_out.shape[1]), BF16),
                vmem((rows, d_model), BF16),
                vmem((1, rows), jnp.int32),
                pltpu.SMEM((rows,), jnp.int32),
                vmem((layers, d_model), BF16),
                vmem((d_model, fused_width), BF16),
                vmem(w_out.shape[1:], BF16),
                vmem((rows, head_dim, seq), BF16),
                vmem((rows, head_dim, seq), BF16),
                vmem((rows, 128), F32),
                vmem((rows, 128), F32),
                vmem((rows, 128), F32),
                vmem((4, rows, 128), F32),
                vmem((rows, 128), F32),
                vmem((rows, 128), F32),
                vmem((rows, d_model), BF16),
                sem((6,)),
                sem((2, n_tiles)),
                sem((2, n_tiles)),
            ],
            compiler_params=pltpu.CompilerParams(vmem_limit_bytes=63 * 1024 * 1024),
            cost_estimate=pl.CostEstimate(flops=10**9, bytes_accessed=10**7, transcendentals=10**6),
            name="first_attention",
        )(hidden, lengths.reshape(1, rows), lengths, keys, values, attn_norm, w_qkv, w_out)
        blocks = pltpu.with_memory_space_constraint(blocks, pltpu.VMEM)
        n_loads = 2 + 5 * layers + 1
        return pl.pallas_call(
            functools.partial(kernel, group, layers, PARTS, 2 * layers),
            out_shape=pltpu.VMEM((rows, d_model), BF16),
            in_specs=[pl.BlockSpec(memory_space=pltpu.VMEM)] + [any_spec] * 11,
            out_specs=pl.BlockSpec(memory_space=pltpu.VMEM),
            scratch_shapes=[
                pltpu.VMEM((rows, d_model), BF16),
                pltpu.VMEM((1, rows), jnp.int32),
                pltpu.VMEM((2, layers, d_model), BF16),
                pltpu.VMEM(w_qkv.shape, BF16),
                pltpu.VMEM(w_out.shape, BF16),
                pltpu.VMEM(w_gate.shape, BF16),
                pltpu.VMEM(w_up.shape, BF16),
                pltpu.VMEM(w_down.shape, BF16),
                pltpu.VMEM((rows, head_dim, seq), BF16),
                pltpu.VMEM((rows, head_dim, seq), BF16),
                pltpu.VMEM((rows, 128), F32),
                pltpu.VMEM((rows, 128), F32),
                pltpu.VMEM((rows, 128), F32),
                pltpu.VMEM((4, rows, 128), F32),
                pltpu.VMEM((rows, 128), F32),
                pltpu.VMEM((rows, 128), F32),
                pltpu.VMEM((rows, w_out.shape[1]), BF16),
                pltpu.VMEM((rows, d_model), BF16),
                pltpu.VMEM((rows, w_down.shape[1]), BF16),
                pltpu.VMEM((PARTS, 4, 2, size, width), BF16),
                pltpu.VMEM((PARTS, group, size, width), BF16),
                pltpu.VMEM((group, rows, width), BF16),
                sem((n_loads,)),
                sem((n_tiles,)),
                sem((n_tiles,)),
                sem((PARTS, 7)),
                sem((PARTS, group)),
                sem((PARTS, 7)),
                sem((PARTS, group)),
            ],
            compiler_params=pltpu.CompilerParams(
                collective_id=0, has_side_effects=True, vmem_limit_bytes=VMEM_MIB * 1024 * 1024),
            cost_estimate=pl.CostEstimate(flops=4 * 10**9, bytes_accessed=64 * 10**6, transcendentals=10**6),
            name="decode_layers",
        )(blocks, hidden, lengths.reshape(1, rows), keys, values, attn_norm, w_qkv, w_out, mlp_norm, w_gate, w_up, w_down)

    cache_spec = P(None, "dp", None, "tp", None)
    in_specs = (P("dp", None), P("dp"), cache_spec, cache_spec, P(), P(None, None, "tp", None),
                P(None, "tp", None), P(), P(None, None, "tp"), P(None, None, "tp"), P(None, "tp", None))
    return jax.shard_map(local_step, mesh=mesh, in_specs=in_specs, out_specs=P("dp", None), check_vma=False)
```
